256 devices in a mesh: dom: 128 (over x, z, y), mem: 2 (over core).
Axes of the slice: x: 4, y: 4, z: 8, core: 2. Of those that a mesh axis runs over, the one named last changes fastest.
Arguments:
- node_latents: bfloat16 [4, 16384, 512], P('mem', 'dom'), may hold values from -6 to 6
- edge_latents: bfloat16 [4, 65536, 512], P('mem', 'dom'), may hold values from -6 to 6
- edge_senders: int32 [65536], P('dom'), may hold values from 0 to 415, as said below
- edge_receivers: int32 [65536], P('dom'), may hold values from 0 to 127
- edge_counts: int32 [128], P('dom'), may hold values from 64 to 512, as said below
- halo_send: int32 [4096], P('dom'), may hold values from 0 to 127
- long_send: int32 [128, 128, 2], replicated, may hold values from 0 to 3
- edge_first: bfloat16 [2, 1536, 512], P(None, None, 'mem'), may hold values from -0.15625 to 0.15625
- edge_second: bfloat16 [2, 512, 512], P(None, None, 'mem'), may hold values from -0.25 to 0.25
- node_first: bfloat16 [2, 1024, 512], P(None, None, 'mem'), may hold values from -0.1875 to 0.1875
- node_second: bfloat16 [2, 512, 512], P(None, None, 'mem'), may hold values from -0.25 to 0.25
- edge_gain: float32 [2, 512], replicated, may hold values from 0.5 to 1.5
- edge_shift: float32 [2, 512], replicated, may hold values from -3 to 3
- node_gain: float32 [2, 512], replicated, may hold values from 0.5 to 1.5
- node_shift: float32 [2, 512], replicated, may hold values from -3 to 3
Outputs:
- node_out: bfloat16 [4, 16384, 512], P('mem', 'dom')
- edge_out: bfloat16 [4, 65536, 512], P('mem', 'dom')
The draws below stay inside these ranges and needn't reach their ends.
Inputs may be any that keep to these rules, and one draw needn't show every extreme that they name: `edge_senders`: rows below 128 are the partition's own nodes, the next 32 its neighbours' sent nodes, the rest the coarse slots of all partitions. `edge_counts`: live slots come first in each partition; some partition has exactly 512 live slots.
All inputs are finite; a program needn't handle non-finite values.
Results may differ from the reference program's by a relative error of at most 0.0075.
Values may be sent and summed in bfloat16 or wider, within the bound.
A program may use at most 128 MiB of HBM per device.

```python
import jax
import jax.numpy as jnp
from jax import lax

D = 512
NODE_DEV = 128
EDGE_DEV = 512
HALO = 16
COARSE_DEV = 4
LONG_SLOT = 2
LAYERS = 2
MEMBERS = 4
NODES = 16384
EDGES = 65536
N_DOM = 128


def draw_edge_senders(key, part):
    kind_key = jax.random.fold_in(key, 11)
    local_key = jax.random.fold_in(key, 12)
    halo_key = jax.random.fold_in(key, 13)
    far_key = jax.random.fold_in(key, 14)
    total = N_DOM * EDGE_DEV
    kinds = jax.random.randint(kind_key, (total,), 0, 20)
    local_rows = jax.random.randint(local_key, (total,), 0, NODE_DEV)
    halo_rows = NODE_DEV + jax.random.randint(halo_key, (total,), 0, 2 * HALO)
    far_rows = NODE_DEV + 2 * HALO + jax.random.randint(far_key, (total,), 0, N_DOM * LONG_SLOT)
    picked = jnp.where(kinds < 14, local_rows, jnp.where(kinds < 17, halo_rows, far_rows))
    return picked.astype(jnp.int32)


def draw_edge_counts(key, part):
    count_key = jax.random.fold_in(key, 21)
    place_key = jax.random.fold_in(key, 22)
    counts = jax.random.randint(count_key, (N_DOM,), EDGE_DEV // 8, EDGE_DEV + 1)
    fullest = jax.random.randint(place_key, (), 0, N_DOM)
    counts = jnp.where(jnp.arange(N_DOM) == fullest, EDGE_DEV, counts)
    return counts.astype(jnp.int32)


def set_ends(values, stream_key, smallest, top_value):
    longest = values.shape.index(max(values.shape))
    spots = []
    for shift in (0, 1):
        where = [jax.random.randint(jax.random.fold_in(stream_key, axis), (), 0, length) for axis, length in enumerate(values.shape)]
        where[longest] = (where[longest] + shift) % values.shape[longest]
        spots.append(tuple(where))
    return values.at[spots[0]].set(smallest).at[spots[1]].set(top_value)


def block_levels(stream_key, dims, pieces, least, high):
    def one(dim, blocks):
        heights = jax.random.uniform(jax.random.fold_in(jax.random.fold_in(stream_key, 6), dim), (blocks,), jnp.float32, least / len(pieces), high / len(pieces))
        return jnp.repeat(jnp.exp(heights), dims[dim] // blocks).reshape((-1,) + (1,) * (len(dims) - dim - 1))

    gain = one(*pieces[0])
    for cut in pieces[1:]:
        gain = gain * one(*cut)
    return gain


def noise(stream_key, shape, deviation, most, shards=(), kind=jnp.bfloat16):
    factor_of = block_levels(stream_key, shape, shards, -0.22, 0.18) if shards else 1.0
    drawn = jax.random.normal(stream_key, shape, jnp.float32) * deviation * factor_of
    return jnp.minimum(jnp.maximum(drawn, -most), most).astype(kind)


def setup_inputs(seed: int = 0) -> dict:
    seeds = jax.random.split(jax.random.key(seed), 16)
    node_latents = noise(seeds[0], (MEMBERS, NODES, D), 1.0, 6.0, ((0, 2), (1, 128)))
    edge_latents = noise(seeds[1], (MEMBERS, EDGES, D), 1.0, 6.0, ((0, 2), (1, 128)))
    edge_senders = draw_edge_senders(jax.random.fold_in(seeds[15], 71), 0)
    edge_receivers = set_ends(jax.random.randint(seeds[3], (EDGES,), 0, NODE_DEV), jax.random.fold_in(seeds[3], 1), 0, NODE_DEV - 1).astype(jnp.int32)
    edge_counts = draw_edge_counts(jax.random.fold_in(seeds[15], 71), 0)
    halo_send = set_ends(jax.random.randint(seeds[5], (N_DOM * 2 * HALO,), 0, NODE_DEV), jax.random.fold_in(seeds[5], 1), 0, NODE_DEV - 1).astype(jnp.int32)
    long_send = set_ends(jax.random.randint(seeds[6], (N_DOM, N_DOM, LONG_SLOT), 0, COARSE_DEV), jax.random.fold_in(seeds[6], 1), 0, COARSE_DEV - 1).astype(jnp.int32)
    edge_first = noise(seeds[7], (LAYERS, 3 * D, D), (3 * D) ** -0.5, 0.15625, ((2, 2),))
    edge_second = noise(seeds[8], (LAYERS, D, D), D ** -0.5, 0.25, ((2, 2),))
    node_first = noise(seeds[9], (LAYERS, 2 * D, D), (2 * D) ** -0.5, 0.1875, ((2, 2),))
    node_second = noise(seeds[10], (LAYERS, D, D), D ** -0.5, 0.25, ((2, 2),))
    edge_gain = jnp.clip(1.0 + 0.1 * jax.random.normal(seeds[11], (LAYERS, D), jnp.float32), 0.5, 1.5)
    edge_shift = noise(seeds[12], (LAYERS, D), 0.5, 3.0, (), jnp.float32)
    node_gain = jnp.clip(1.0 + 0.1 * jax.random.normal(seeds[13], (LAYERS, D), jnp.float32), 0.5, 1.5)
    node_shift = noise(seeds[14], (LAYERS, D), 0.5, 3.0, (), jnp.float32)
    return {"node_latents": node_latents, "edge_latents": edge_latents, "edge_senders": edge_senders, "edge_receivers": edge_receivers, "edge_counts": edge_counts, "halo_send": halo_send, "long_send": long_send, "edge_first": edge_first, "edge_second": edge_second, "node_first": node_first, "node_second": node_second, "edge_gain": edge_gain, "edge_shift": edge_shift, "node_gain": node_gain, "node_shift": node_shift}


def project_norm(inputs, first_weight, second, scale_gain, offset):
    hidden = jax.nn.silu(jnp.dot(inputs, first_weight, preferred_element_type=jnp.float32)).astype(jnp.bfloat16)
    output = jnp.dot(hidden, second, preferred_element_type=jnp.float32)
    average = lax.optimization_barrier(jnp.mean(output, -1, keepdims=True))
    centred = output - average
    variance = lax.optimization_barrier(jnp.mean(centred * centred, -1, keepdims=True))
    return centred * lax.rsqrt(variance + 1e-05) * scale_gain + offset

def reference(node_latents, edge_latents, edge_senders, edge_receivers, edge_counts, halo_send, long_send, edge_first, edge_second, node_first, node_second, edge_gain, edge_shift, node_gain, node_shift):
    partitions = N_DOM
    node_rows = NODE_DEV
    edge_rows = EDGE_DEV
    features = D
    members = node_latents.shape[0]
    halo_rows = halo_send.reshape(partitions, 2 * HALO)
    partition_ids = jnp.arange(partitions, dtype=jnp.int32)
    own_ids = partition_ids[:, None] * node_rows + jnp.arange(node_rows, dtype=jnp.int32)[None, :]
    previous = (partition_ids - 1) % partitions
    following = (partition_ids + 1) % partitions
    left_ids = previous[:, None] * node_rows + halo_rows[previous][:, HALO:]
    right_ids = following[:, None] * node_rows + halo_rows[following][:, :HALO]
    far_ids = partition_ids[None, :, None] * node_rows + jnp.transpose(long_send, (1, 0, 2))
    far_ids = far_ids.reshape(partitions, partitions * LONG_SLOT)
    source_ids = jnp.concatenate([own_ids, left_ids, right_ids, far_ids], 1).astype(jnp.int32)
    senders = edge_senders.reshape(partitions, edge_rows)
    sender_ids = jnp.take_along_axis(source_ids, senders, axis=1)
    receivers = edge_receivers.reshape(partitions, edge_rows)
    node_state = node_latents
    edge_state = jnp.transpose(edge_latents.reshape(members, partitions, edge_rows, features), (1, 0, 2, 3))
    for layer_index in range(LAYERS):

        def one_part(part_item):
            snd_ids, rcv_ids, live_count, edge_block, node_block = part_item
            sender_rows = jnp.take(node_state, snd_ids, axis=1)
            receiver_rows = jnp.take(node_block, rcv_ids, axis=1)
            joined = jnp.concatenate([edge_block, sender_rows, receiver_rows], -1).reshape(members * edge_rows, 3 * features)
            update = project_norm(joined, edge_first[layer_index], edge_second[layer_index], edge_gain[layer_index], edge_shift[layer_index]).reshape(members, edge_rows, features)
            live_mask = jnp.arange(edge_rows, dtype=jnp.int32) < live_count
            new_edges = jnp.where(live_mask[None, :, None], edge_block.astype(jnp.float32) + update, 0.0).astype(jnp.bfloat16)
            onehot = ((rcv_ids[None, :] == jnp.arange(node_rows, dtype=jnp.int32)[:, None]) & live_mask[None, :]).astype(jnp.float32)
            summed = jnp.einsum('ne,med->mnd', onehot, new_edges.astype(jnp.float32)).astype(jnp.bfloat16)
            node_in = jnp.concatenate([node_block, summed], -1).reshape(members * node_rows, 2 * features)
            node_update = project_norm(node_in, node_first[layer_index], node_second[layer_index], node_gain[layer_index], node_shift[layer_index]).reshape(members, node_rows, features)
            new_nodes = (node_block.astype(jnp.float32) + node_update).astype(jnp.bfloat16)
            return (new_nodes, new_edges)
        node_blocks = jnp.transpose(node_state.reshape(members, partitions, node_rows, features), (1, 0, 2, 3))
        new_nodes, new_edges = lax.map(one_part, (sender_ids, receivers, edge_counts, edge_state, node_blocks))
        node_state = jnp.transpose(new_nodes, (1, 0, 2, 3)).reshape(members, partitions * node_rows, features)
        edge_state = new_edges
    edge_final = jnp.transpose(edge_state, (1, 0, 2, 3)).reshape(members, partitions * edge_rows, features)
    return (node_state, edge_final)
```

```python
import functools

import jax
import jax.numpy as jnp
from jax import lax
from jax.experimental import pallas as pl
from jax.experimental.pallas import tpu as pltpu
from jax.sharding import PartitionSpec as P

NX, NZ, NY = 4, 8, 4
HALO = 16
LAYERS = 2
COARSE = 4
MESH = pl.DeviceIdType.MESH
F32 = jnp.float32
BF16 = jnp.bfloat16
RING = sorted(range(1, NZ), key=lambda d: -min(d, NZ - d))
PLANE = sorted(
    [(i, j) for i in range(NX) for j in range(NY) if (i, j) != (0, 0)],
    key=lambda o: -(min(o[0], NX - o[0]) + min(o[1], NY - o[1])),
)


def dot(a, b):
    return jnp.dot(a, b, preferred_element_type=F32)


def silu(x):
    half = 0.5 * x
    return half * jnp.tanh(half) + half


def kernel(
    dims,
    count_ref,
    senders_ref,
    receivers_ref,
    halo_ref,
    pick_ref,
    eg_ref,
    eb_ref,
    ng_ref,
    nb_ref,
    node_hbm,
    edge_hbm,
    ef_hbm,
    es_hbm,
    nf_hbm,
    ns_hbm,
    node_out,
    edge_out,
    node_v,
    edge_v,
    w1e,
    w2e,
    w1n,
    w2n,
    near_rows,
    far_rows,
    ring_send,
    ring_recv,
    plane_send,
    halo_out,
    o_near,
    o_far,
    o_recv,
    o_sum,
    o_pick,
    o_pack,
    pre_v,
    hid_v,
    load_sem,
    out_sem,
    w_send,
    w_recv,
    ring_ssem,
    ring_rsem,
    plane_ssem,
    plane_rsem,
    halo_ssem,
    halo_rsem,
):
    M, N, E, D = dims
    H = D // 2
    K = N + 2 * HALO
    dom = lax.axis_index("dom")
    mem = lax.axis_index("mem")
    y = lax.rem(dom, NY)
    z = lax.rem(lax.div(dom, NY), NZ)
    x = lax.div(dom, NY * NZ)

    def dom_of(a, b, c):
        return (a * NZ + b) * NY + c

    def along(d):
        return (dom_of(x, lax.rem(z + d, NZ), y), mem)

    def across(o):
        return (dom_of(lax.rem(x + o[0], NX), z, lax.rem(y + o[1], NY)), mem)

    nd = NX * NY * NZ
    after = (lax.rem(dom + 1, nd), mem)
    before = (lax.rem(dom + nd - 1, nd), mem)
    twin = (dom, 1 - mem)
    here = x * NY + y
    peers = [along(d) for d in RING] + [across(o) for o in PLANE] + [after, before, twin]
    barrier = pltpu.get_barrier_semaphore()
    for p in peers:
        pl.semaphore_signal(barrier, inc=1, device_id=p, device_id_type=MESH)

    weights = ((ef_hbm, w1e), (es_hbm, w2e), (nf_hbm, w1n), (ns_hbm, w2n))
    node_load = pltpu.make_async_copy(node_hbm, node_v, load_sem.at[0])
    edge_load = pltpu.make_async_copy(edge_hbm, edge_v, load_sem.at[1])
    node_load.start()
    w_load = {}
    for l in range(LAYERS):
        for i, (src, dst) in enumerate(weights):
            w_load[l, i] = pltpu.make_async_copy(
                src.at[l], dst.at[l, mem], load_sem.at[2 + 4 * l + i]
            )
            w_load[l, i].start()
            if l == 0 and i == 0:
                edge_load.start()

    live = count_ref[0]
    table = lax.broadcasted_iota(jnp.int32, (K, E), 0)
    sent = senders_ref[...]
    o_near[...] = jnp.where(table == sent, 1.0, 0.0).T.astype(BF16)
    q = jnp.maximum(sent - K, 0)
    slot = lax.rem(q, 2)
    part = lax.div(q, 2)
    part_y = lax.rem(part, NY)
    part_z = lax.rem(lax.div(part, NY), NZ)
    part_x = lax.div(part, NY * NZ)
    place = jnp.where(
        sent >= K, (part_x * NY + part_y) * (2 * NZ) + part_z * 2 + slot, -1
    )
    F = 2 * nd
    table = lax.broadcasted_iota(jnp.int32, (F, E), 0)
    o_far[...] = jnp.where(table == place, 1.0, 0.0).T.astype(BF16)
    table = lax.broadcasted_iota(jnp.int32, (N, E), 0)
    lane = lax.broadcasted_iota(jnp.int32, (N, E), 1)
    got = jnp.where((table == receivers_ref[...]) & (lane < live), 1.0, 0.0)
    o_sum[...] = got.astype(BF16)
    o_recv[...] = got.T.astype(BF16)
    row = lax.broadcasted_iota(jnp.int32, (N, 2 * HALO), 0)
    halo = jnp.where(row == halo_ref[...], 1.0, 0.0).T
    row = lax.broadcasted_iota(jnp.int32, (8, N), 0)
    col = lax.broadcasted_iota(jnp.int32, (8, N), 1)
    o_pack[0] = jnp.where(row == col, jnp.where(row < COARSE, 1.0, 0.0), 0.0).astype(BF16)
    o_pack[1] = jnp.where(row == col + COARSE, 1.0, 0.0).astype(BF16)
    o_halo = halo.astype(BF16)
    G = NX * NY * 2 * NZ
    table = lax.broadcasted_iota(jnp.int32, (8 * NZ, G), 0)
    o_pick[0] = jnp.where(table == pick_ref[...], 1.0, 0.0).T.astype(BF16)
    o_pick[1] = jnp.where(table == pick_ref[...] + COARSE, 1.0, 0.0).T.astype(BF16)

    def ring_copy(l, m, d):
        return pltpu.make_async_remote_copy(
            src_ref=ring_send.at[l, m],
            dst_ref=ring_recv.at[l, m, z],
            send_sem=ring_ssem.at[l, m, d],
            recv_sem=ring_rsem.at[l, m, d],
            device_id=along(d),
            device_id_type=MESH,
        )

    def plane_copy(l, m, k):
        o = PLANE[k]
        there = lax.rem(x + o[0], NX) * NY + lax.rem(y + o[1], NY)
        return pltpu.make_async_remote_copy(
            src_ref=plane_send.at[l, m, there],
            dst_ref=far_rows.at[l, m, here],
            send_sem=plane_ssem.at[l, m, k],
            recv_sem=plane_rsem.at[l, m, k],
            device_id=across(o),
            device_id_type=MESH,
        )

    def halo_copy(l, m, side):
        return pltpu.make_async_remote_copy(
            src_ref=halo_out.at[l, m, side],
            dst_ref=near_rows.at[l, m, pl.ds(N + (1 - side) * HALO, HALO)],
            send_sem=halo_ssem.at[l, m, side],
            recv_sem=halo_rsem.at[l, m, side],
            device_id=before if side == 0 else after,
            device_id_type=MESH,
        )

    def weight_copy(l, i):
        src, dst = weights[i]
        return pltpu.make_async_remote_copy(
            src_ref=src.at[l],
            dst_ref=dst.at[l, mem],
            send_sem=w_send.at[l, i],
            recv_sem=w_recv.at[l, i],
            device_id=twin,
            device_id_type=MESH,
        )

    def pack(l, m):
        rows = near_rows[l, m, 0:N]
        ring_send[l, m] = (
            dot(o_pack[0], rows[:, 0:H]) + dot(o_pack[1], rows[:, H:D])
        ).astype(BF16)
        return rows

    def halo_pack(l, m, rows):
        out = dot(o_halo, rows).astype(BF16)
        halo_out[l, m, 0] = out[0:HALO]
        halo_out[l, m, 1] = out[HALO : 2 * HALO]

    def ring_start(l, m):
        ring_recv[l, m, z] = ring_send[l, m]
        for d in RING:
            ring_copy(l, m, d).start()

    def halo_start(l, m):
        for side in range(2):
            halo_copy(l, m, side).start()

    def forward(l, m):
        for d in RING:
            ring_copy(l, m, d).wait_recv()
        got = ring_recv[l, m].reshape(8 * NZ, H)
        for h in range(2):
            plane_send[l, m, :, :, h * H : (h + 1) * H] = (
                dot(o_pick[h], got).astype(BF16).reshape(NX * NY, 2 * NZ, H)
            )
        for k in range(len(PLANE)):
            plane_copy(l, m, k).start()
        far_rows[l, m, here] = plane_send[l, m, here]

    def halo_wait(l, m):
        for side in range(2):
            halo_copy(l, m, side).wait_recv()

    def near(l, m):
        rows = near_rows[l, m]
        for n in range(2):
            cols = slice(n * H, (n + 1) * H)
            proj = dot(rows, w1e[l, n, D : 2 * D]).astype(BF16)
            own = dot(rows[0:N], w1e[l, n, 2 * D : 3 * D]).astype(BF16)
            pre_v[m, :, cols] = (
                dot(edge_v[m], w1e[l, n, 0:D])
                + dot(o_near[...], proj)
                + dot(o_recv[...], own)
            )

    def norm(v, gain, shift):
        mean = jnp.mean(v, -1, keepdims=True)
        c = v - mean
        var = jnp.mean(c * c, -1, keepdims=True)
        return c * lax.rsqrt(var + 1e-05) * gain + shift

    CH = min(256, E)

    def edges(l, m):
        for k in range(len(PLANE)):
            plane_copy(l, m, k).wait_recv()
        rows = far_rows[l, m].reshape(F, D)
        for n in range(2):
            cols = slice(n * H, (n + 1) * H)
            proj = dot(rows, w1e[l, n, D : 2 * D]).astype(BF16)
            for c in range(E // CH):
                r = slice(c * CH, (c + 1) * CH)
                hid_v[r, cols] = silu(pre_v[m, r, cols] + dot(o_far[r], proj)).astype(BF16)
        gain = eg_ref[l : l + 1]
        shift = eb_ref[l : l + 1]
        for c in range(E // CH):
            r = slice(c * CH, (c + 1) * CH)
            h = hid_v[r]
            v = jnp.concatenate([dot(h, w2e[l, 0]), dot(h, w2e[l, 1])], -1)
            u = norm(v, gain, shift)
            at = lax.broadcasted_iota(jnp.int32, (CH, 1), 0) + c * CH
            edge_v[m, r] = jnp.where(
                at < live, edge_v[m, r].astype(F32) + u, 0.0
            ).astype(BF16)

    def nodes(l, m):
        summed = dot(o_sum[...], edge_v[m]).astype(BF16)
        rows = near_rows[l, m, 0:N]
        hid = []
        for n in range(2):
            a = dot(rows, w1n[l, n, 0:D]) + dot(summed, w1n[l, n, D : 2 * D])
            hid.append(silu(a).astype(BF16))
        h = jnp.concatenate(hid, -1)
        v = jnp.concatenate([dot(h, w2n[l, 0]), dot(h, w2n[l, 1])], -1)
        u = norm(v, ng_ref[l : l + 1], nb_ref[l : l + 1])
        return (rows.astype(F32) + u).astype(BF16)

    node_load.wait()
    for m in range(M):
        near_rows[0, m, 0:N] = node_v[m]
        rows = pack(0, m)
        halo_pack(0, m, rows)
    pl.semaphore_wait(barrier, len(peers))
    for m in range(M):
        ring_start(0, m)
    for m in range(M):
        halo_start(0, m)
    for l in range(LAYERS):
        for i in range(4):
            weight_copy(l, i).start()
    for m in range(M):
        forward(0, m)
    edge_load.wait()
    for l in range(LAYERS):
        for i in range(4):
            if l == 0:
                w_load[l, i].wait()
    weight_copy(0, 0).wait_recv()
    for m in range(M):
        halo_wait(0, m)
        near(0, m)
    for i in range(1, 4):
        weight_copy(0, i).wait_recv()
    for m in range(M):
        edges(0, m)
        new = nodes(0, m)
        near_rows[1, m, 0:N] = new
        rows = pack(1, m)
        ring_start(1, m)
        halo_pack(1, m, rows)
        halo_start(1, m)
    for i in range(4):
        w_load[1, i].wait()
        weight_copy(1, i).wait_recv()
    halo_wait(1, 0)
    near(1, 0)
    forward(1, 0)
    halo_wait(1, 1)
    near(1, 1)
    forward(1, 1)
    outs = []
    for m in range(M):
        edges(1, m)
        out = pltpu.make_async_copy(edge_v.at[m], edge_out.at[m], out_sem.at[m, 0])
        out.start()
        outs.append(out)
        node_v[m] = nodes(1, m)
        out = pltpu.make_async_copy(node_v.at[m], node_out.at[m], out_sem.at[m, 1])
        out.start()
        outs.append(out)
    for l in range(LAYERS):
        for i in range(4):
            weight_copy(l, i).wait_send()
        for m in range(M):
            for d in RING:
                ring_copy(l, m, d).wait_send()
            for k in range(len(PLANE)):
                plane_copy(l, m, k).wait_send()
            for side in range(2):
                halo_copy(l, m, side).wait_send()
    for out in outs:
        out.wait()


def per_device(
    node_latents,
    edge_latents,
    edge_senders,
    edge_receivers,
    edge_counts,
    halo_send,
    long_send,
    edge_first,
    edge_second,
    node_first,
    node_second,
    edge_gain,
    edge_shift,
    node_gain,
    node_shift,
):
    M, N, D = node_latents.shape
    E = edge_latents.shape[1]
    H = D // 2
    L = LAYERS
    nd = NX * NY * NZ
    K = N + 2 * HALO
    F = 2 * nd
    G = NX * NY * 2 * NZ
    dom = lax.axis_index("dom")
    y = lax.rem(dom, NY)
    z = lax.rem(lax.div(dom, NY), NZ)
    x = lax.div(dom, NY * NZ)
    sent = long_send.transpose(0, 2, 1).reshape(NX, NZ, NY, 2, NX, NZ, NY)
    sent = lax.dynamic_slice(
        sent, (x, 0, y, 0, 0, z, 0), (1, NZ, 1, 2, NX, 1, NY)
    ).reshape(NZ, 2, NX * NY)
    pick = sent.transpose(2, 0, 1) + 8 * jnp.arange(NZ, dtype=jnp.int32)[None, :, None]
    pick = pick.reshape(1, G)
    vmem = pl.BlockSpec(memory_space=pltpu.VMEM)
    smem = pl.BlockSpec(memory_space=pltpu.SMEM)
    hbm = pl.BlockSpec(memory_space=pl.ANY)
    DMA = pltpu.SemaphoreType.DMA
    return pl.pallas_call(
        functools.partial(kernel, (M, N, E, D)),
        out_shape=(
            jax.ShapeDtypeStruct((M, N, D), BF16),
            jax.ShapeDtypeStruct((M, E, D), BF16),
        ),
        in_specs=[smem] + [vmem] * 8 + [hbm] * 6,
        out_specs=(hbm, hbm),
        scratch_shapes=[
            pltpu.VMEM((M, N, D), BF16),
            pltpu.VMEM((M, E, D), BF16),
            pltpu.VMEM((L, 2, 3 * D, H), BF16),
            pltpu.VMEM((L, 2, D, H), BF16),
            pltpu.VMEM((L, 2, 2 * D, H), BF16),
            pltpu.VMEM((L, 2, D, H), BF16),
            pltpu.VMEM((L, M, K, D), BF16),
            pltpu.VMEM((L, M, NX * NY, 2 * NZ, D), BF16),
            pltpu.VMEM((L, M, 8, H), BF16),
            pltpu.VMEM((L, M, NZ, 8, H), BF16),
            pltpu.VMEM((L, M, NX * NY, 2 * NZ, D), BF16),
            pltpu.VMEM((L, M, 2, HALO, D), BF16),
            pltpu.VMEM((E, K), BF16),
            pltpu.VMEM((E, F), BF16),
            pltpu.VMEM((E, N), BF16),
            pltpu.VMEM((N, E), BF16),
            pltpu.VMEM((2, G, 8 * NZ), BF16),
            pltpu.VMEM((2, 8, N), BF16),
            pltpu.VMEM((M, E, D), F32),
            pltpu.VMEM((E, D), BF16),
            DMA((2 + 4 * L,)),
            DMA((M, 2)),
            DMA((L, 4)),
            DMA((L, 4)),
            DMA((L, M, NZ)),
            DMA((L, M, NZ)),
            DMA((L, M, len(PLANE))),
            DMA((L, M, len(PLANE))),
            DMA((L, M, 2)),
            DMA((L, M, 2)),
        ],
        compiler_params=pltpu.CompilerParams(
            collective_id=0, has_side_effects=True, vmem_limit_bytes=56 * 1024 * 1024
        ),
    )(
        edge_counts,
        edge_senders.reshape(1, E),
        edge_receivers.reshape(1, E),
        halo_send.reshape(1, 2 * HALO),
        pick,
        edge_gain,
        edge_shift,
        node_gain,
        node_shift,
        node_latents,
        edge_latents,
        edge_first,
        edge_second,
        node_first,
        node_second,
    )


def solution(mesh):
    placed = (
        P("mem", "dom", None),
        P("mem", "dom", None),
        P("dom"),
        P("dom"),
        P("dom"),
        P("dom"),
        P(),
        P(None, None, "mem"),
        P(None, None, "mem"),
        P(None, None, "mem"),
        P(None, None, "mem"),
        P(),
        P(),
        P(),
        P(),
    )
    return jax.shard_map(
        per_device,
        mesh=mesh,
        in_specs=placed,
        out_specs=(P("mem", "dom", None), P("mem", "dom", None)),
        check_vma=False,
    )
```

```python
import functools

import jax
import jax.numpy as jnp
from jax import lax
from jax.experimental import pallas as pl
from jax.experimental.pallas import tpu as pltpu
from jax.sharding import PartitionSpec as P

NX, NZ, NY = 4, 8, 4
HALO = 16
LAYERS = 2
COARSE = 4
MESH = pl.DeviceIdType.MESH
F32 = jnp.float32
BF16 = jnp.bfloat16
RING = sorted(range(1, NZ), key=lambda d: -min(d, NZ - d))
PLANE = sorted(
    [(i, j) for i in range(NX) for j in range(NY) if (i, j) != (0, 0)],
    key=lambda o: -(min(o[0], NX - o[0]) + min(o[1], NY - o[1])),
)


def dot(a, b):
    return jnp.dot(a, b, preferred_element_type=F32)


def silu(x):
    half = 0.5 * x
    return half * jnp.tanh(half) + half


def kernel(
    dims,
    count_ref,
    senders_hbm,
    receivers_hbm,
    halo_hbm,
    eg_hbm,
    eb_hbm,
    ng_hbm,
    nb_hbm,
    long_hbm,
    node_hbm,
    edge_hbm,
    ef_hbm,
    es_hbm,
    nf_hbm,
    ns_hbm,
    node_out,
    edge_out,
    node_v,
    edge_v,
    long_v,
    senders_ref,
    receivers_ref,
    halo_ref,
    eg_ref,
    eb_ref,
    ng_ref,
    nb_ref,
    w1e,
    w2e,
    w1n,
    w2n,
    near_rows,
    far_rows,
    ring_send,
    ring_recv,
    plane_send,
    halo_out,
    o_near,
    o_far,
    o_recv,
    o_sum,
    o_pick,
    o_pack,
    pre_v,
    hid_v,
    load_sem,
    long_sem,
    small_sem,
    out_sem,
    w_send,
    w_recv,
    ring_ssem,
    ring_rsem,
    plane_ssem,
    plane_rsem,
    halo_ssem,
    halo_rsem,
):
    M, N, E, D = dims
    H = D // 2
    K = N + 2 * HALO
    dom = lax.axis_index("dom")
    mem = lax.axis_index("mem")
    y = lax.rem(dom, NY)
    z = lax.rem(lax.div(dom, NY), NZ)
    x = lax.div(dom, NY * NZ)

    def dom_of(a, b, c):
        return (a * NZ + b) * NY + c

    def along(d):
        return (dom_of(x, lax.rem(z + d, NZ), y), mem)

    def across(o):
        return (dom_of(lax.rem(x + o[0], NX), z, lax.rem(y + o[1], NY)), mem)

    nd = NX * NY * NZ
    after = (lax.rem(dom + 1, nd), mem)
    before = (lax.rem(dom + nd - 1, nd), mem)
    twin = (dom, 1 - mem)
    here = x * NY + y
    peers = [along(d) for d in RING] + [across(o) for o in PLANE] + [after, before, twin]
    barrier = pltpu.get_barrier_semaphore()
    for p in peers:
        pl.semaphore_signal(barrier, inc=1, device_id=p, device_id_type=MESH)

    weights = ((ef_hbm, w1e), (es_hbm, w2e), (nf_hbm, w1n), (ns_hbm, w2n))
    long_load = [
        pltpu.make_async_copy(
            long_hbm.at[dom_of(x, i, y)], long_v.at[pl.ds(2 * i, 2)], long_sem.at[i]
        )
        for i in range(NZ)
    ]
    small = (
        (senders_hbm, senders_ref),
        (receivers_hbm, receivers_ref),
        (halo_hbm, halo_ref),
        (eg_hbm, eg_ref),
        (eb_hbm, eb_ref),
        (ng_hbm, ng_ref),
        (nb_hbm, nb_ref),
    )
    small_load = [
        pltpu.make_async_copy(src, dst, small_sem.at[i])
        for i, (src, dst) in enumerate(small)
    ]
    for copy in small_load + long_load:
        copy.start()
    node_load = pltpu.make_async_copy(node_hbm, node_v, load_sem.at[0])
    edge_load = pltpu.make_async_copy(edge_hbm, edge_v, load_sem.at[1])
    node_load.start()
    w_load = {}
    for l in range(LAYERS):
        for i, (src, dst) in enumerate(weights):
            w_load[l, i] = pltpu.make_async_copy(
                src.at[l], dst.at[l, mem], load_sem.at[2 + 4 * l + i]
            )
            w_load[l, i].start()
            if l == 0 and i == 0:
                edge_load.start()

    for copy in small_load:
        copy.wait()
    live = count_ref[0]
    table = lax.broadcasted_iota(jnp.int32, (K, E), 0)
    sent = senders_ref[...]
    o_near[...] = jnp.where(table == sent, 1.0, 0.0).T.astype(BF16)
    q = jnp.maximum(sent - K, 0)
    slot = lax.rem(q, 2)
    part = lax.div(q, 2)
    part_y = lax.rem(part, NY)
    part_z = lax.rem(lax.div(part, NY), NZ)
    part_x = lax.div(part, NY * NZ)
    place = jnp.where(
        sent >= K, (part_x * NY + part_y) * (2 * NZ) + part_z * 2 + slot, -1
    )
    F = 2 * nd
    table = lax.broadcasted_iota(jnp.int32, (F, E), 0)
    o_far[...] = jnp.where(table == place, 1.0, 0.0).T.astype(BF16)
    table = lax.broadcasted_iota(jnp.int32, (N, E), 0)
    lane = lax.broadcasted_iota(jnp.int32, (N, E), 1)
    got = jnp.where((table == receivers_ref[...]) & (lane < live), 1.0, 0.0)
    o_sum[...] = got.astype(BF16)
    o_recv[...] = got.T.astype(BF16)
    row = lax.broadcasted_iota(jnp.int32, (N, 2 * HALO), 0)
    halo = jnp.where(row == halo_ref[...], 1.0, 0.0).T
    row = lax.broadcasted_iota(jnp.int32, (8, N), 0)
    col = lax.broadcasted_iota(jnp.int32, (8, N), 1)
    o_pack[0] = jnp.where(row == col, jnp.where(row < COARSE, 1.0, 0.0), 0.0).astype(BF16)
    o_pack[1] = jnp.where(row == col + COARSE, 1.0, 0.0).astype(BF16)
    o_halo = halo.astype(BF16)
    G = NX * NY * 2 * NZ
    row = lax.broadcasted_iota(jnp.int32, (G, nd), 0)
    col = lax.broadcasted_iota(jnp.int32, (G, nd), 1)
    to = lax.div(row, 2 * NZ)
    want = dom_of(lax.div(to, NY), z, lax.rem(to, NY))
    spread = jnp.where(col == want, 1.0, 0.0).astype(BF16)
    for copy in long_load:
        copy.wait()
    coarse = long_v[...].astype(F32).astype(BF16)
    every = lax.dot_general(
        spread, coarse, (((1,), (1,)), ((), ())), preferred_element_type=F32
    )
    row = lax.broadcasted_iota(jnp.int32, (G, 2 * NZ), 0)
    col = lax.broadcasted_iota(jnp.int32, (G, 2 * NZ), 1)
    mine = jnp.where(col == lax.rem(row, 2 * NZ), every, 0.0).astype(BF16)
    pick = dot(mine, jnp.ones((2 * NZ, 8 * NZ), BF16))
    row = lax.broadcasted_iota(jnp.int32, (G, 8 * NZ), 0)
    col = lax.broadcasted_iota(jnp.int32, (G, 8 * NZ), 1)
    pick = pick + (8 * lax.div(lax.rem(row, 2 * NZ), 2)).astype(F32)
    for h in range(2):
        o_pick[h] = jnp.where(
            col.astype(F32) == pick + float(COARSE * h), 1.0, 0.0
        ).astype(BF16)

    def ring_copy(l, m, d):
        return pltpu.make_async_remote_copy(
            src_ref=ring_send.at[l, m],
            dst_ref=ring_recv.at[l, m, z],
            send_sem=ring_ssem.at[l, m, d],
            recv_sem=ring_rsem.at[l, m, d],
            device_id=along(d),
            device_id_type=MESH,
        )

    def plane_copy(l, m, k):
        o = PLANE[k]
        there = lax.rem(x + o[0], NX) * NY + lax.rem(y + o[1], NY)
        return pltpu.make_async_remote_copy(
            src_ref=plane_send.at[l, m, there],
            dst_ref=far_rows.at[l, m, here],
            send_sem=plane_ssem.at[l, m, k],
            recv_sem=plane_rsem.at[l, m, k],
            device_id=across(o),
            device_id_type=MESH,
        )

    def halo_copy(l, m, side):
        return pltpu.make_async_remote_copy(
            src_ref=halo_out.at[l, m, side],
            dst_ref=near_rows.at[l, m, pl.ds(N + (1 - side) * HALO, HALO)],
            send_sem=halo_ssem.at[l, m, side],
            recv_sem=halo_rsem.at[l, m, side],
            device_id=before if side == 0 else after,
            device_id_type=MESH,
        )

    def weight_copy(l, i):
        src, dst = weights[i]
        return pltpu.make_async_remote_copy(
            src_ref=src.at[l],
            dst_ref=dst.at[l, mem],
            send_sem=w_send.at[l, i],
            recv_sem=w_recv.at[l, i],
            device_id=twin,
            device_id_type=MESH,
        )

    def pack(l, m):
        rows = near_rows[l, m, 0:N]
        ring_send[l, m] = (
            dot(o_pack[0], rows[:, 0:H]) + dot(o_pack[1], rows[:, H:D])
        ).astype(BF16)
        return rows

    def halo_pack(l, m, rows):
        out = dot(o_halo, rows).astype(BF16)
        halo_out[l, m, 0] = out[0:HALO]
        halo_out[l, m, 1] = out[HALO : 2 * HALO]

    def ring_start(l, m):
        ring_recv[l, m, z] = ring_send[l, m]
        for d in RING:
            ring_copy(l, m, d).start()

    def halo_start(l, m):
        for side in range(2):
            halo_copy(l, m, side).start()

    def forward(l, m):
        for d in RING:
            ring_copy(l, m, d).wait_recv()
        got = ring_recv[l, m].reshape(8 * NZ, H)
        for h in range(2):
            plane_send[l, m, :, :, h * H : (h + 1) * H] = (
                dot(o_pick[h], got).astype(BF16).reshape(NX * NY, 2 * NZ, H)
            )
        for k in range(len(PLANE)):
            plane_copy(l, m, k).start()
        far_rows[l, m, here] = plane_send[l, m, here]

    def halo_wait(l, m):
        for side in range(2):
            halo_copy(l, m, side).wait_recv()

    def near(l, m):
        rows = near_rows[l, m]
        for n in range(2):
            cols = slice(n * H, (n + 1) * H)
            proj = dot(rows, w1e[l, n, D : 2 * D]).astype(BF16)
            own = dot(rows[0:N], w1e[l, n, 2 * D : 3 * D]).astype(BF16)
            pre_v[m, :, cols] = (
                dot(edge_v[m], w1e[l, n, 0:D])
                + dot(o_near[...], proj)
                + dot(o_recv[...], own)
            )

    def norm(v, gain, shift):
        mean = jnp.mean(v, -1, keepdims=True)
        c = v - mean
        var = jnp.mean(c * c, -1, keepdims=True)
        return c * lax.rsqrt(var + 1e-05) * gain + shift

    CH = min(256, E)

    def edges(l, m):
        for k in range(len(PLANE)):
            plane_copy(l, m, k).wait_recv()
        rows = far_rows[l, m].reshape(F, D)
        for n in range(2):
            cols = slice(n * H, (n + 1) * H)
            proj = dot(rows, w1e[l, n, D : 2 * D]).astype(BF16)
            for c in range(E // CH):
                r = slice(c * CH, (c + 1) * CH)
                hid_v[r, cols] = silu(pre_v[m, r, cols] + dot(o_far[r], proj)).astype(BF16)
        gain = eg_ref[l : l + 1]
        shift = eb_ref[l : l + 1]
        for c in range(E // CH):
            r = slice(c * CH, (c + 1) * CH)
            h = hid_v[r]
            v = jnp.concatenate([dot(h, w2e[l, 0]), dot(h, w2e[l, 1])], -1)
            u = norm(v, gain, shift)
            at = lax.broadcasted_iota(jnp.int32, (CH, 1), 0) + c * CH
            edge_v[m, r] = jnp.where(
                at < live, edge_v[m, r].astype(F32) + u, 0.0
            ).astype(BF16)

    def nodes(l, m):
        summed = dot(o_sum[...], edge_v[m]).astype(BF16)
        rows = near_rows[l, m, 0:N]
        hid = []
        for n in range(2):
            a = dot(rows, w1n[l, n, 0:D]) + dot(summed, w1n[l, n, D : 2 * D])
            hid.append(silu(a).astype(BF16))
        h = jnp.concatenate(hid, -1)
        v = jnp.concatenate([dot(h, w2n[l, 0]), dot(h, w2n[l, 1])], -1)
        u = norm(v, ng_ref[l : l + 1], nb_ref[l : l + 1])
        return (rows.astype(F32) + u).astype(BF16)

    node_load.wait()
    for m in range(M):
        near_rows[0, m, 0:N] = node_v[m]
        rows = pack(0, m)
        halo_pack(0, m, rows)
    pl.semaphore_wait(barrier, len(peers))
    for m in range(M):
        ring_start(0, m)
    for m in range(M):
        halo_start(0, m)
    for l in range(LAYERS):
        for i in range(4):
            weight_copy(l, i).start()
    for m in range(M):
        forward(0, m)
    edge_load.wait()
    for l in range(LAYERS):
        for i in range(4):
            if l == 0:
                w_load[l, i].wait()
    weight_copy(0, 0).wait_recv()
    for m in range(M):
        halo_wait(0, m)
        near(0, m)
    for i in range(1, 4):
        weight_copy(0, i).wait_recv()
    for m in range(M):
        edges(0, m)
        new = nodes(0, m)
        near_rows[1, m, 0:N] = new
        rows = pack(1, m)
        ring_start(1, m)
        halo_pack(1, m, rows)
        halo_start(1, m)
    for i in range(4):
        w_load[1, i].wait()
        weight_copy(1, i).wait_recv()
    halo_wait(1, 0)
    near(1, 0)
    forward(1, 0)
    halo_wait(1, 1)
    near(1, 1)
    forward(1, 1)
    outs = []
    for m in range(M):
        edges(1, m)
        out = pltpu.make_async_copy(edge_v.at[m], edge_out.at[m], out_sem.at[m, 0])
        out.start()
        outs.append(out)
        node_v[m] = nodes(1, m)
        out = pltpu.make_async_copy(node_v.at[m], node_out.at[m], out_sem.at[m, 1])
        out.start()
        outs.append(out)
    for l in range(LAYERS):
        for i in range(4):
            weight_copy(l, i).wait_send()
        for m in range(M):
            for d in RING:
                ring_copy(l, m, d).wait_send()
            for k in range(len(PLANE)):
                plane_copy(l, m, k).wait_send()
            for side in range(2):
                halo_copy(l, m, side).wait_send()
    for out in outs:
        out.wait()


def per_device(
    node_latents,
    edge_latents,
    edge_senders,
    edge_receivers,
    edge_counts,
    halo_send,
    long_send,
    edge_first,
    edge_second,
    node_first,
    node_second,
    edge_gain,
    edge_shift,
    node_gain,
    node_shift,
):
    M, N, D = node_latents.shape
    E = edge_latents.shape[1]
    H = D // 2
    L = LAYERS
    nd = NX * NY * NZ
    K = N + 2 * HALO
    F = 2 * nd
    G = NX * NY * 2 * NZ
    smem = pl.BlockSpec(memory_space=pltpu.SMEM)
    hbm = pl.BlockSpec(memory_space=pl.ANY)
    DMA = pltpu.SemaphoreType.DMA
    return pl.pallas_call(
        functools.partial(kernel, (M, N, E, D)),
        out_shape=(
            jax.ShapeDtypeStruct((M, N, D), BF16),
            jax.ShapeDtypeStruct((M, E, D), BF16),
        ),
        in_specs=[smem] + [hbm] * 14,
        out_specs=(hbm, hbm),
        scratch_shapes=[
            pltpu.VMEM((M, N, D), BF16),
            pltpu.VMEM((M, E, D), BF16),
            pltpu.VMEM((2 * NZ, nd), jnp.int32),
            pltpu.VMEM((1, E), jnp.int32),
            pltpu.VMEM((1, E), jnp.int32),
            pltpu.VMEM((1, 2 * HALO), jnp.int32),
            pltpu.VMEM((L, D), F32),
            pltpu.VMEM((L, D), F32),
            pltpu.VMEM((L, D), F32),
            pltpu.VMEM((L, D), F32),
            pltpu.VMEM((L, 2, 3 * D, H), BF16),
            pltpu.VMEM((L, 2, D, H), BF16),
            pltpu.VMEM((L, 2, 2 * D, H), BF16),
            pltpu.VMEM((L, 2, D, H), BF16),
            pltpu.VMEM((L, M, K, D), BF16),
            pltpu.VMEM((L, M, NX * NY, 2 * NZ, D), BF16),
            pltpu.VMEM((L, M, 8, H), BF16),
            pltpu.VMEM((L, M, NZ, 8, H), BF16),
            pltpu.VMEM((L, M, NX * NY, 2 * NZ, D), BF16),
            pltpu.VMEM((L, M, 2, HALO, D), BF16),
            pltpu.VMEM((E, K), BF16),
            pltpu.VMEM((E, F), BF16),
            pltpu.VMEM((E, N), BF16),
            pltpu.VMEM((N, E), BF16),
            pltpu.VMEM((2, G, 8 * NZ), BF16),
            pltpu.VMEM((2, 8, N), BF16),
            pltpu.VMEM((M, E, D), F32),
            pltpu.VMEM((E, D), BF16),
            DMA((2 + 4 * L,)),
            DMA((NZ,)),
            DMA((7,)),
            DMA((M, 2)),
            DMA((L, 4)),
            DMA((L, 4)),
            DMA((L, M, NZ)),
            DMA((L, M, NZ)),
            DMA((L, M, len(PLANE))),
            DMA((L, M, len(PLANE))),
            DMA((L, M, 2)),
            DMA((L, M, 2)),
        ],
        compiler_params=pltpu.CompilerParams(
            collective_id=0, has_side_effects=True, vmem_limit_bytes=56 * 1024 * 1024
        ),
    )(
        edge_counts,
        edge_senders.reshape(1, E),
        edge_receivers.reshape(1, E),
        halo_send.reshape(1, 2 * HALO),
        edge_gain,
        edge_shift,
        node_gain,
        node_shift,
        long_send.transpose(0, 2, 1),
        node_latents,
        edge_latents,
        edge_first,
        edge_second,
        node_first,
        node_second,
    )


def solution(mesh):
    placed = (
        P("mem", "dom", None),
        P("mem", "dom", None),
        P("dom"),
        P("dom"),
        P("dom"),
        P("dom"),
        P(),
        P(None, None, "mem"),
        P(None, None, "mem"),
        P(None, None, "mem"),
        P(None, None, "mem"),
        P(),
        P(),
        P(),
        P(),
    )
    return jax.shard_map(
        per_device,
        mesh=mesh,
        in_specs=placed,
        out_specs=(P("mem", "dom", None), P("mem", "dom", None)),
        check_vma=False,
    )
```

```python
import functools

import jax
import jax.numpy as jnp
from jax import lax
from jax.experimental import pallas as pl
from jax.experimental.pallas import tpu as pltpu
from jax.sharding import PartitionSpec as P

NX, NZ, NY = 4, 8, 4
HALO = 16
LAYERS = 2
COARSE = 4
MESH = pl.DeviceIdType.MESH
F32 = jnp.float32
BF16 = jnp.bfloat16
RING = sorted(range(NZ), key=lambda d: (min(d, NZ - d), d))
BATCHES = (2, 1)
PLANE = sorted(
    [(i, j) for i in range(NX) for j in range(NY) if (i, j) != (0, 0)],
    key=lambda o: -(min(o[0], NX - o[0]) + min(o[1], NY - o[1])),
)


def dot(a, b):
    return jnp.dot(a, b, preferred_element_type=F32)


def silu(x):
    half = 0.5 * x
    return half * jnp.tanh(half) + half


def kernel(
    dims,
    count_hbm,
    senders_hbm,
    receivers_hbm,
    halo_hbm,
    eg_hbm,
    eb_hbm,
    ng_hbm,
    nb_hbm,
    long_hbm,
    node_hbm,
    edge_hbm,
    ef_hbm,
    es_hbm,
    nf_hbm,
    ns_hbm,
    node_out,
    edge_out,
    node_v,
    edge_v,
    head_v,
    long_v,
    count_ref,
    senders_ref,
    receivers_ref,
    halo_ref,
    eg_ref,
    eb_ref,
    ng_ref,
    nb_ref,
    w1e,
    w2e,
    w1n,
    w2n,
    near_rows,
    far_rows,
    ring_send,
    ring_recv,
    plane_send,
    halo_out,
    o_near,
    o_far,
    o_recv,
    o_sum,
    o_halo,
    o_pick_one,
    o_pick_two,
    pre_v,
    node_pre,
    hid_v,
    head_sem,
    load_sem,
    long_sem,
    small_sem,
    out_sem,
    w_send,
    w_recv,
    ring_ssem,
    ring_rsem,
    plane_ssem,
    plane_rsem,
    halo_ssem,
    halo_rsem,
):
    M, N, E, D = dims
    H = D // 2
    K = N + 2 * HALO
    dom = lax.axis_index("dom")
    mem = lax.axis_index("mem")
    y = lax.rem(dom, NY)
    z = lax.rem(lax.div(dom, NY), NZ)
    x = lax.div(dom, NY * NZ)

    def dom_of(a, b, c):
        return (a * NZ + b) * NY + c

    def along(d):
        return (dom_of(x, lax.rem(z + d, NZ), y), mem)

    def across(o):
        return (dom_of(lax.rem(x + o[0], NX), z, lax.rem(y + o[1], NY)), mem)

    nd = NX * NY * NZ
    after = (lax.rem(dom + 1, nd), mem)
    before = (lax.rem(dom + nd - 1, nd), mem)
    twin = (dom, 1 - mem)
    here = x * NY + y
    peers = [along(d) for d in RING[1:]] + [across(o) for o in PLANE]
    peers += [after, before, twin]
    barrier = pltpu.get_barrier_semaphore()
    for p in peers:
        pl.semaphore_signal(barrier, inc=1, device_id=p, device_id_type=MESH)

    weights = ((ef_hbm, w1e), (es_hbm, w2e), (nf_hbm, w1n), (ns_hbm, w2n))
    long_load = [
        pltpu.make_async_copy(
            long_hbm.at[dom_of(x, lax.rem(z + NZ - d, NZ), y)],
            long_v.at[pl.ds(2 * k, 2)],
            long_sem.at[k],
        )
        for k, d in enumerate(RING)
    ]
    small = (
        (count_hbm, count_ref),
        (senders_hbm, senders_ref),
        (receivers_hbm, receivers_ref),
        (halo_hbm, halo_ref),
        (eg_hbm, eg_ref),
        (eb_hbm, eb_ref),
        (ng_hbm, ng_ref),
        (nb_hbm, nb_ref),
    )
    small_load = [
        pltpu.make_async_copy(src, dst, small_sem.at[i])
        for i, (src, dst) in enumerate(small)
    ]
    for copy in small_load + long_load:
        copy.start()
    node_load = pltpu.make_async_copy(node_hbm, node_v, load_sem.at[0])
    edge_load = pltpu.make_async_copy(edge_hbm, edge_v, load_sem.at[1])
    head_load = pltpu.make_async_copy(node_hbm.at[:, pl.ds(0, 8)], head_v, head_sem)
    head_load.start()
    node_load.start()
    w_load = {}
    for l in range(LAYERS):
        for i, (src, dst) in enumerate(weights):
            w_load[l, i] = pltpu.make_async_copy(
                src.at[l], dst.at[l, mem], load_sem.at[2 + 4 * l + i]
            )
            w_load[l, i].start()
            if l == 0 and i == 0:
                edge_load.start()

    F = 2 * nd

    def ring_copy(l, m, k):
        return pltpu.make_async_remote_copy(
            src_ref=ring_send.at[l, m],
            dst_ref=ring_recv.at[l, m, k],
            send_sem=ring_ssem.at[l, m, k],
            recv_sem=ring_rsem.at[l, m, k],
            device_id=along(RING[k]),
            device_id_type=MESH,
        )

    def plane_copy(l, m, b, k):
        o = PLANE[k]
        there = lax.rem(x + o[0], NX) * NY + lax.rem(y + o[1], NY)
        rows = 2 * NZ // BATCHES[l]
        return pltpu.make_async_remote_copy(
            src_ref=plane_send.at[l, m, there, pl.ds(b * rows, rows)],
            dst_ref=far_rows.at[l, m, here, pl.ds(b * rows, rows)],
            send_sem=plane_ssem.at[l, m, b, k],
            recv_sem=plane_rsem.at[l, m, b, k],
            device_id=across(o),
            device_id_type=MESH,
        )

    def halo_copy(l, m, side):
        return pltpu.make_async_remote_copy(
            src_ref=halo_out.at[l, m, side],
            dst_ref=near_rows.at[l, m, pl.ds(N + (1 - side) * HALO, HALO)],
            send_sem=halo_ssem.at[l, m, side],
            recv_sem=halo_rsem.at[l, m, side],
            device_id=before if side == 0 else after,
            device_id_type=MESH,
        )

    def weight_copy(l, i):
        src, dst = weights[i]
        return pltpu.make_async_remote_copy(
            src_ref=src.at[l],
            dst_ref=dst.at[l, mem],
            send_sem=w_send.at[l, i],
            recv_sem=w_recv.at[l, i],
            device_id=twin,
            device_id_type=MESH,
        )

    def pack(l, m, rows):
        wide = rows.astype(F32)
        upper = pltpu.roll(wide[:, H:D], COARSE, 0)
        row = lax.broadcasted_iota(jnp.int32, (8, H), 0)
        packed = jnp.where(row < COARSE, wide[:, 0:H], upper).astype(BF16)
        ring_send[l, m] = packed
        ring_recv[l, m, 0] = packed

    def halo_pack(l, m, rows):
        out = dot(o_halo[...], rows).astype(BF16)
        halo_out[l, m, 0] = out[0:HALO]
        halo_out[l, m, 1] = out[HALO : 2 * HALO]

    def ring_start(l, m):
        for k in reversed(range(1, NZ)):
            ring_copy(l, m, k).start()

    def halo_start(l, m):
        for side in range(2):
            halo_copy(l, m, side).start()

    def forward(l, m, b):
        nb = BATCHES[l]
        o_pick = o_pick_one if nb == 1 else o_pick_two
        size = NZ // nb
        for k in range(max(b * size, 1), (b + 1) * size):
            ring_copy(l, m, k).wait_recv()
        got = ring_recv[l, m, b * size : (b + 1) * size].reshape(8 * size, H)
        S = 2 * size
        rows = slice(b * NX * NY * S, (b + 1) * NX * NY * S)
        for h in range(2):
            plane_send[l, m, :, b * S : (b + 1) * S, h * H : (h + 1) * H] = (
                dot(o_pick[h, rows], got).astype(BF16).reshape(NX * NY, S, H)
            )
        for k in range(len(PLANE)):
            plane_copy(l, m, b, k).start()
        far_rows[l, m, here, b * S : (b + 1) * S] = plane_send[
            l, m, here, b * S : (b + 1) * S
        ]

    def halo_wait(l, m):
        for side in range(2):
            halo_copy(l, m, side).wait_recv()

    def own_part(l, m):
        rows = near_rows[l, m, 0:N]
        for n in range(2):
            cols = slice(n * H, (n + 1) * H)
            own = dot(rows, w1e[l, n, 2 * D : 3 * D]).astype(BF16)
            pre_v[m, :, cols] = dot(edge_v[m], w1e[l, n, 0:D]) + dot(o_recv[...], own)

    def near_part(l, m):
        rows = near_rows[l, m]
        for n in range(2):
            cols = slice(n * H, (n + 1) * H)
            proj = dot(rows, w1e[l, n, D : 2 * D]).astype(BF16)
            pre_v[m, :, cols] += dot(o_near[...], proj)

    def node_part(l, m):
        rows = near_rows[l, m, 0:N]
        for n in range(2):
            node_pre[m, :, n * H : (n + 1) * H] = dot(rows, w1n[l, n, 0:D])

    def norm(v, gain, shift):
        mean = jnp.mean(v, -1, keepdims=True)
        c = v - mean
        var = jnp.mean(c * c, -1, keepdims=True)
        return c * lax.rsqrt(var + 1e-05) * gain + shift

    CH = min(256, E)

    def edges(l, m):
        for b in range(BATCHES[l]):
            for k in range(len(PLANE)):
                plane_copy(l, m, b, k).wait_recv()
        rows = far_rows[l, m].reshape(F, D)
        for n in range(2):
            cols = slice(n * H, (n + 1) * H)
            proj = dot(rows, w1e[l, n, D : 2 * D]).astype(BF16)
            for c in range(E // CH):
                r = slice(c * CH, (c + 1) * CH)
                hid_v[r, cols] = silu(pre_v[m, r, cols] + dot(o_far[r], proj)).astype(BF16)
        gain = eg_ref[l : l + 1]
        shift = eb_ref[l : l + 1]
        for c in range(E // CH):
            r = slice(c * CH, (c + 1) * CH)
            h = hid_v[r]
            v = jnp.concatenate([dot(h, w2e[l, 0]), dot(h, w2e[l, 1])], -1)
            u = norm(v, gain, shift)
            at = lax.broadcasted_iota(jnp.int32, (CH, 1), 0) + c * CH
            edge_v[m, r] = jnp.where(
                at < live, edge_v[m, r].astype(F32) + u, 0.0
            ).astype(BF16)

    def nodes(l, m):
        summed = dot(o_sum[...], edge_v[m]).astype(BF16)
        rows = near_rows[l, m, 0:N]
        hid = []
        for n in range(2):
            a = node_pre[m, :, n * H : (n + 1) * H] + dot(summed, w1n[l, n, D : 2 * D])
            hid.append(silu(a).astype(BF16))
        h = jnp.concatenate(hid, -1)
        v = jnp.concatenate([dot(h, w2n[l, 0]), dot(h, w2n[l, 1])], -1)
        u = norm(v, ng_ref[l : l + 1], nb_ref[l : l + 1])
        return (rows.astype(F32) + u).astype(BF16)

    head_load.wait()
    for m in range(M):
        pack(0, m, head_v[m])
    pl.semaphore_wait(barrier, len(peers))
    for m in range(M):
        ring_start(0, m)
    for copy in small_load:
        copy.wait()
    row = lax.broadcasted_iota(jnp.int32, (N, 2 * HALO), 0)
    halo = jnp.where(row == halo_ref[...], 1.0, 0.0).T
    o_halo[...] = halo.astype(BF16)
    node_load.wait()
    for m in range(M):
        rows = node_v[m]
        near_rows[0, m, 0:N] = rows
        halo_pack(0, m, rows)
        halo_start(0, m)
    for l in range(LAYERS):
        for i in range(4):
            weight_copy(l, i).start()
    for copy in long_load:
        copy.wait()
    coarse = long_v[...].astype(F32).astype(BF16)
    G = NX * NY * 2 * NZ
    for nb, o_pick in ((1, o_pick_one), (2, o_pick_two)):
        S = 2 * NZ // nb
        row = lax.broadcasted_iota(jnp.int32, (G, nd), 0)
        col = lax.broadcasted_iota(jnp.int32, (G, nd), 1)
        to = lax.rem(lax.div(row, S), NX * NY)
        want = dom_of(lax.div(to, NY), z, lax.rem(to, NY))
        spread = jnp.where(col == want, 1.0, 0.0).astype(BF16)
        every = lax.dot_general(
            spread, coarse, (((1,), (1,)), ((), ())), preferred_element_type=F32
        )
        row = lax.broadcasted_iota(jnp.int32, (G, 2 * NZ), 0)
        col = lax.broadcasted_iota(jnp.int32, (G, 2 * NZ), 1)
        own = lax.div(row, NX * NY * S) * S + lax.rem(row, S)
        mine = jnp.where(col == own, every, 0.0).astype(BF16)
        pick = dot(mine, jnp.ones((2 * NZ, 4 * S), BF16))
        row = lax.broadcasted_iota(jnp.int32, (G, 4 * S), 0)
        col = lax.broadcasted_iota(jnp.int32, (G, 4 * S), 1)
        pick = pick + (8 * lax.div(lax.rem(row, S), 2)).astype(F32)
        for h in range(2):
            o_pick[h] = jnp.where(
                col.astype(F32) == pick + float(COARSE * h), 1.0, 0.0
            ).astype(BF16)

    live = count_ref[0]
    table = lax.broadcasted_iota(jnp.int32, (K, E), 0)
    sent = senders_ref[...]
    o_near[...] = jnp.where(table == sent, 1.0, 0.0).T.astype(BF16)
    q = jnp.maximum(sent - K, 0)
    slot = lax.rem(q, 2)
    part = lax.div(q, 2)
    part_y = lax.rem(part, NY)
    part_z = lax.rem(lax.div(part, NY), NZ)
    part_x = lax.div(part, NY * NZ)
    apart = lax.rem(z + NZ - part_z, NZ)
    rank = jnp.zeros_like(apart)
    for k, d in enumerate(RING):
        rank = jnp.where(apart == d, k, rank)
    place = (part_x * NY + part_y) * (2 * NZ) + rank * 2 + slot
    place = jnp.where(sent >= K, place, -1)
    table = lax.broadcasted_iota(jnp.int32, (F, E), 0)
    o_far[...] = jnp.where(table == place, 1.0, 0.0).T.astype(BF16)
    table = lax.broadcasted_iota(jnp.int32, (N, E), 0)
    lane = lax.broadcasted_iota(jnp.int32, (N, E), 1)
    got = jnp.where((table == receivers_ref[...]) & (lane < live), 1.0, 0.0)
    o_sum[...] = got.astype(BF16)
    o_recv[...] = got.T.astype(BF16)
    for b in range(BATCHES[0]):
        for m in range(M):
            forward(0, m, b)
    edge_load.wait()
    for i in range(4):
        w_load[0, i].wait()
    weight_copy(0, 0).wait_recv()
    for m in range(M):
        own_part(0, m)
    for m in range(M):
        halo_wait(0, m)
        near_part(0, m)
    for i in range(1, 4):
        weight_copy(0, i).wait_recv()
    for m in range(M):
        node_part(0, m)
    for m in range(M):
        edges(0, m)
        new = nodes(0, m)
        pack(1, m, new[0:8])
        ring_start(1, m)
        near_rows[1, m, 0:N] = new
        halo_pack(1, m, new)
        halo_start(1, m)
    for i in range(4):
        w_load[1, i].wait()
        weight_copy(1, i).wait_recv()
    own_part(1, 0)
    forward(1, 0, 0)
    own_part(1, 1)
    node_part(1, 0)
    forward(1, 1, 0)
    node_part(1, 1)
    halo_wait(1, 0)
    near_part(1, 0)
    halo_wait(1, 1)
    near_part(1, 1)
    outs = []
    for m in range(M):
        edges(1, m)
        out = pltpu.make_async_copy(edge_v.at[m], edge_out.at[m], out_sem.at[m, 0])
        out.start()
        outs.append(out)
        node_v[m] = nodes(1, m)
        out = pltpu.make_async_copy(node_v.at[m], node_out.at[m], out_sem.at[m, 1])
        out.start()
        outs.append(out)
    for l in range(LAYERS):
        for i in range(4):
            weight_copy(l, i).wait_send()
        for m in range(M):
            for k in range(1, NZ):
                ring_copy(l, m, k).wait_send()
            for b in range(BATCHES[l]):
                for k in range(len(PLANE)):
                    plane_copy(l, m, b, k).wait_send()
            for side in range(2):
                halo_copy(l, m, side).wait_send()
    for out in outs:
        out.wait()


def publish(node_in, edge_in, node_out, edge_out, node_v, edge_v, in_sem, out_sem):
    M, E = edge_in.shape[:2]
    pieces = []
    for m in range(M):
        for h in range(2):
            rows = pl.ds(h * (E // 2), E // 2)
            pieces.append(
                (edge_in.at[m, rows], edge_v.at[2 * m + h], edge_out.at[m, rows])
            )
    pieces.append((node_in, node_v, node_out))
    ins = [
        pltpu.make_async_copy(a, b, in_sem.at[i]) for i, (a, b, c) in enumerate(pieces)
    ]
    outs = [
        pltpu.make_async_copy(b, c, out_sem.at[i]) for i, (a, b, c) in enumerate(pieces)
    ]
    for copy in ins:
        copy.start()
    for a, b in zip(ins, outs):
        a.wait()
        b.start()
    for copy in outs:
        copy.wait()


def per_device(
    node_latents,
    edge_latents,
    edge_senders,
    edge_receivers,
    edge_counts,
    halo_send,
    long_send,
    edge_first,
    edge_second,
    node_first,
    node_second,
    edge_gain,
    edge_shift,
    node_gain,
    node_shift,
):
    M, N, D = node_latents.shape
    E = edge_latents.shape[1]
    H = D // 2
    L = LAYERS
    nd = NX * NY * NZ
    K = N + 2 * HALO
    F = 2 * nd
    G = NX * NY * 2 * NZ
    hbm = pl.BlockSpec(memory_space=pl.ANY)
    DMA = pltpu.SemaphoreType.DMA
    node_state, edge_state = pl.pallas_call(
        functools.partial(kernel, (M, N, E, D)),
        out_shape=(
            jax.ShapeDtypeStruct((M, N, D), BF16),
            jax.ShapeDtypeStruct((M, E, D), BF16),
        ),
        in_specs=[hbm] * 15,
        out_specs=(hbm, hbm),
        scratch_shapes=[
            pltpu.VMEM((M, N, D), BF16),
            pltpu.VMEM((M, E, D), BF16),
            pltpu.VMEM((M, 8, D), BF16),
            pltpu.VMEM((2 * NZ, nd), jnp.int32),
            pltpu.SMEM((1,), jnp.int32),
            pltpu.VMEM((1, E), jnp.int32),
            pltpu.VMEM((1, E), jnp.int32),
            pltpu.VMEM((1, 2 * HALO), jnp.int32),
            pltpu.VMEM((L, D), F32),
            pltpu.VMEM((L, D), F32),
            pltpu.VMEM((L, D), F32),
            pltpu.VMEM((L, D), F32),
            pltpu.VMEM((L, 2, 3 * D, H), BF16),
            pltpu.VMEM((L, 2, D, H), BF16),
            pltpu.VMEM((L, 2, 2 * D, H), BF16),
            pltpu.VMEM((L, 2, D, H), BF16),
            pltpu.VMEM((L, M, K, D), BF16),
            pltpu.VMEM((L, M, NX * NY, 2 * NZ, D), BF16),
            pltpu.VMEM((L, M, 8, H), BF16),
            pltpu.VMEM((L, M, NZ, 8, H), BF16),
            pltpu.VMEM((L, M, NX * NY, 2 * NZ, D), BF16),
            pltpu.VMEM((L, M, 2, HALO, D), BF16),
            pltpu.VMEM((E, K), BF16),
            pltpu.VMEM((E, F), BF16),
            pltpu.VMEM((E, N), BF16),
            pltpu.VMEM((N, E), BF16),
            pltpu.VMEM((2 * HALO, N), BF16),
            pltpu.VMEM((2, G, 8 * NZ), BF16),
            pltpu.VMEM((2, G, 4 * NZ), BF16),
            pltpu.VMEM((M, E, D), F32),
            pltpu.VMEM((M, N, D), F32),
            pltpu.VMEM((E, D), BF16),
            DMA(()),
            DMA((2 + 4 * L,)),
            DMA((NZ,)),
            DMA((8,)),
            DMA((M, 2)),
            DMA((L, 4)),
            DMA((L, 4)),
            DMA((L, M, NZ)),
            DMA((L, M, NZ)),
            DMA((L, M, 2, len(PLANE))),
            DMA((L, M, 2, len(PLANE))),
            DMA((L, M, 2)),
            DMA((L, M, 2)),
        ],
        compiler_params=pltpu.CompilerParams(
            collective_id=0, has_side_effects=True, vmem_limit_bytes=56 * 1024 * 1024
        ),
    )(
        edge_counts,
        edge_senders.reshape(1, E),
        edge_receivers.reshape(1, E),
        halo_send.reshape(1, 2 * HALO),
        edge_gain,
        edge_shift,
        node_gain,
        node_shift,
        long_send.transpose(0, 2, 1),
        node_latents,
        edge_latents,
        edge_first,
        edge_second,
        node_first,
        node_second,
    )
    return pl.pallas_call(
        publish,
        out_shape=(
            jax.ShapeDtypeStruct((M, N, D), BF16),
            jax.ShapeDtypeStruct((M, E, D), BF16),
        ),
        in_specs=[hbm, hbm],
        out_specs=(hbm, hbm),
        scratch_shapes=[
            pltpu.VMEM((M, N, D), BF16),
            pltpu.VMEM((2 * M, E // 2, D), BF16),
            DMA((1 + 2 * M,)),
            DMA((1 + 2 * M,)),
        ],
    )(node_state, edge_state)


def solution(mesh):
    placed = (
        P("mem", "dom", None),
        P("mem", "dom", None),
        P("dom"),
        P("dom"),
        P("dom"),
        P("dom"),
        P(),
        P(None, None, "mem"),
        P(None, None, "mem"),
        P(None, None, "mem"),
        P(None, None, "mem"),
        P(),
        P(),
        P(),
        P(),
    )
    return jax.shard_map(
        per_device,
        mesh=mesh,
        in_specs=placed,
        out_specs=(P("mem", "dom", None), P("mem", "dom", None)),
        check_vma=False,
    )
```

```python
import functools

import jax
import jax.numpy as jnp
from jax import lax
from jax.experimental import pallas as pl
from jax.experimental.pallas import tpu as pltpu
from jax.sharding import PartitionSpec as P

NX, NZ, NY = 4, 8, 4
HALO = 16
LAYERS = 2
COARSE = 4
MESH = pl.DeviceIdType.MESH
F32 = jnp.float32
BF16 = jnp.bfloat16
RING = sorted(range(NZ), key=lambda d: (min(d, NZ - d), d))
BATCHES = (2, 1)
PLANE = sorted(
    [(i, j) for i in range(NX) for j in range(NY) if (i, j) != (0, 0)],
    key=lambda o: -(min(o[0], NX - o[0]) + min(o[1], NY - o[1])),
)


def dot(a, b):
    return jnp.dot(a, b, preferred_element_type=F32)


def silu(x):
    half = 0.5 * x
    return half * jnp.tanh(half) + half


def kernel(
    dims,
    count_hbm,
    senders_hbm,
    receivers_hbm,
    halo_hbm,
    eg_hbm,
    eb_hbm,
    ng_hbm,
    nb_hbm,
    long_hbm,
    node_hbm,
    edge_hbm,
    ef_hbm,
    es_hbm,
    nf_hbm,
    ns_hbm,
    node_out,
    edge_out,
    node_v,
    edge_v,
    head_v,
    long_v,
    count_ref,
    senders_ref,
    receivers_ref,
    halo_ref,
    eg_ref,
    eb_ref,
    ng_ref,
    nb_ref,
    w1e,
    w2e,
    w1n,
    w2n,
    near_rows,
    far_rows,
    ring_send,
    ring_recv,
    plane_send,
    halo_out,
    o_near,
    o_far,
    o_recv,
    o_sum,
    o_halo,
    o_pick_one,
    o_pick_two,
    pre_v,
    node_pre,
    hid_v,
    head_sem,
    load_sem,
    long_sem,
    small_sem,
    out_sem,
    w_send,
    w_recv,
    ring_ssem,
    ring_rsem,
    plane_ssem,
    plane_rsem,
    halo_ssem,
    halo_rsem,
):
    M, N, E, D = dims
    H = D // 2
    K = N + 2 * HALO
    dom = lax.axis_index("dom")
    mem = lax.axis_index("mem")
    y = lax.rem(dom, NY)
    z = lax.rem(lax.div(dom, NY), NZ)
    x = lax.div(dom, NY * NZ)

    def dom_of(a, b, c):
        return (a * NZ + b) * NY + c

    def along(d):
        return (dom_of(x, lax.rem(z + d, NZ), y), mem)

    def across(o):
        return (dom_of(lax.rem(x + o[0], NX), z, lax.rem(y + o[1], NY)), mem)

    nd = NX * NY * NZ
    after = (lax.rem(dom + 1, nd), mem)
    before = (lax.rem(dom + nd - 1, nd), mem)
    twin = (dom, 1 - mem)
    here = x * NY + y
    peers = [along(d) for d in RING[1:]] + [across(o) for o in PLANE]
    peers += [after, before, twin]
    barrier = pltpu.get_barrier_semaphore()
    for p in peers:
        pl.semaphore_signal(barrier, inc=1, device_id=p, device_id_type=MESH)

    weights = ((ef_hbm, w1e), (es_hbm, w2e), (nf_hbm, w1n), (ns_hbm, w2n))
    long_load = [
        pltpu.make_async_copy(
            long_hbm.at[dom_of(x, lax.rem(z + NZ - d, NZ), y)],
            long_v.at[pl.ds(2 * k, 2)],
            long_sem.at[k],
        )
        for k, d in enumerate(RING)
    ]
    small = (
        (count_hbm, count_ref),
        (senders_hbm, senders_ref),
        (receivers_hbm, receivers_ref),
        (halo_hbm, halo_ref),
        (eg_hbm, eg_ref),
        (eb_hbm, eb_ref),
        (ng_hbm, ng_ref),
        (nb_hbm, nb_ref),
    )
    small_load = [
        pltpu.make_async_copy(src, dst, small_sem.at[i])
        for i, (src, dst) in enumerate(small)
    ]
    for copy in small_load + long_load:
        copy.start()
    node_load = pltpu.make_async_copy(node_hbm, node_v, load_sem.at[0])
    edge_load = pltpu.make_async_copy(edge_hbm, edge_v, load_sem.at[1])
    head_load = pltpu.make_async_copy(node_hbm.at[:, pl.ds(0, 8)], head_v, head_sem)
    head_load.start()
    node_load.start()
    w_load = {}
    for l in range(LAYERS):
        for i, (src, dst) in enumerate(weights):
            w_load[l, i] = pltpu.make_async_copy(
                src.at[l], dst.at[l, mem], load_sem.at[2 + 4 * l + i]
            )
            w_load[l, i].start()
            if l == 0 and i == 0:
                edge_load.start()

    F = 2 * nd

    def ring_copy(l, m, k):
        return pltpu.make_async_remote_copy(
            src_ref=ring_send.at[l, m],
            dst_ref=ring_recv.at[l, m, k],
            send_sem=ring_ssem.at[l, m, k],
            recv_sem=ring_rsem.at[l, m, k],
            device_id=along(RING[k]),
            device_id_type=MESH,
        )

    def plane_copy(l, m, b, k):
        o = PLANE[k]
        there = lax.rem(x + o[0], NX) * NY + lax.rem(y + o[1], NY)
        rows = 2 * NZ // BATCHES[l]
        return pltpu.make_async_remote_copy(
            src_ref=plane_send.at[l, m, there, pl.ds(b * rows, rows)],
            dst_ref=far_rows.at[l, m, here, pl.ds(b * rows, rows)],
            send_sem=plane_ssem.at[l, m, b, k],
            recv_sem=plane_rsem.at[l, m, b, k],
            device_id=across(o),
            device_id_type=MESH,
        )

    def halo_copy(l, m, side):
        return pltpu.make_async_remote_copy(
            src_ref=halo_out.at[l, m, side],
            dst_ref=near_rows.at[l, m, pl.ds(N + (1 - side) * HALO, HALO)],
            send_sem=halo_ssem.at[l, m, side],
            recv_sem=halo_rsem.at[l, m, side],
            device_id=before if side == 0 else after,
            device_id_type=MESH,
        )

    def weight_copy(l, i):
        src, dst = weights[i]
        return pltpu.make_async_remote_copy(
            src_ref=src.at[l],
            dst_ref=dst.at[l, mem],
            send_sem=w_send.at[l, i],
            recv_sem=w_recv.at[l, i],
            device_id=twin,
            device_id_type=MESH,
        )

    def pack(l, m, rows):
        wide = rows.astype(F32)
        upper = pltpu.roll(wide[:, H:D], COARSE, 0)
        row = lax.broadcasted_iota(jnp.int32, (8, H), 0)
        packed = jnp.where(row < COARSE, wide[:, 0:H], upper).astype(BF16)
        ring_send[l, m] = packed
        ring_recv[l, m, 0] = packed

    def halo_pack(l, m, rows):
        out = dot(o_halo[...], rows).astype(BF16)
        halo_out[l, m, 0] = out[0:HALO]
        halo_out[l, m, 1] = out[HALO : 2 * HALO]

    def ring_start(l, m):
        for k in reversed(range(1, NZ)):
            ring_copy(l, m, k).start()

    def halo_start(l, m):
        for side in range(2):
            halo_copy(l, m, side).start()

    def forward(l, m, b):
        nb = BATCHES[l]
        o_pick = o_pick_one if nb == 1 else o_pick_two
        size = NZ // nb
        for k in range(max(b * size, 1), (b + 1) * size):
            ring_copy(l, m, k).wait_recv()
        got = ring_recv[l, m, b * size : (b + 1) * size].reshape(8 * size, H)
        S = 2 * size
        rows = slice(b * NX * NY * S, (b + 1) * NX * NY * S)
        for h in range(2):
            plane_send[l, m, :, b * S : (b + 1) * S, h * H : (h + 1) * H] = (
                dot(o_pick[h, rows], got).astype(BF16).reshape(NX * NY, S, H)
            )
        for k in range(len(PLANE)):
            plane_copy(l, m, b, k).start()
        far_rows[l, m, here, b * S : (b + 1) * S] = plane_send[
            l, m, here, b * S : (b + 1) * S
        ]

    def halo_wait(l, m):
        for side in range(2):
            halo_copy(l, m, side).wait_recv()

    def own_part(l, m):
        rows = near_rows[l, m, 0:N]
        for n in range(2):
            cols = slice(n * H, (n + 1) * H)
            own = dot(rows, w1e[l, n, 2 * D : 3 * D]).astype(BF16)
            pre_v[m, :, cols] = dot(edge_v[m], w1e[l, n, 0:D]) + dot(o_recv[...], own)

    def near_part(l, m):
        rows = near_rows[l, m]
        for n in range(2):
            cols = slice(n * H, (n + 1) * H)
            proj = dot(rows, w1e[l, n, D : 2 * D]).astype(BF16)
            pre_v[m, :, cols] += dot(o_near[...], proj)

    def node_part(l, m):
        rows = near_rows[l, m, 0:N]
        for n in range(2):
            node_pre[m, :, n * H : (n + 1) * H] = dot(rows, w1n[l, n, 0:D])

    def norm(v, gain, shift):
        var = jnp.mean(v * v, -1, keepdims=True)
        return v * lax.rsqrt(var + 1e-05) * gain + shift

    def centre(l, w):
        a, b = w[l, 0].astype(F32), w[l, 1].astype(F32)
        mean = jnp.sum(a + b, -1, keepdims=True) * (1.0 / D)
        w[l, 0] = (a - mean).astype(BF16)
        w[l, 1] = (b - mean).astype(BF16)

    CH = min(256, E)

    def edges(l, m):
        for b in range(BATCHES[l]):
            for k in range(len(PLANE)):
                plane_copy(l, m, b, k).wait_recv()
        rows = far_rows[l, m].reshape(F, D)
        for n in range(2):
            cols = slice(n * H, (n + 1) * H)
            proj = dot(rows, w1e[l, n, D : 2 * D]).astype(BF16)
            for c in range(E // CH):
                r = slice(c * CH, (c + 1) * CH)
                hid_v[r, cols] = silu(pre_v[m, r, cols] + dot(o_far[r], proj)).astype(BF16)
        gain = eg_ref[l : l + 1]
        shift = eb_ref[l : l + 1]
        for c in range(E // CH):
            r = slice(c * CH, (c + 1) * CH)
            h = hid_v[r]
            v = jnp.concatenate([dot(h, w2e[l, 0]), dot(h, w2e[l, 1])], -1)
            u = norm(v, gain, shift)
            at = lax.broadcasted_iota(jnp.int32, (CH, 1), 0) + c * CH
            edge_v[m, r] = jnp.where(
                at < live, edge_v[m, r].astype(F32) + u, 0.0
            ).astype(BF16)

    def nodes(l, m):
        summed = dot(o_sum[...], edge_v[m]).astype(BF16)
        rows = near_rows[l, m, 0:N]
        hid = []
        for n in range(2):
            a = node_pre[m, :, n * H : (n + 1) * H] + dot(summed, w1n[l, n, D : 2 * D])
            hid.append(silu(a).astype(BF16))
        h = jnp.concatenate(hid, -1)
        v = jnp.concatenate([dot(h, w2n[l, 0]), dot(h, w2n[l, 1])], -1)
        u = norm(v, ng_ref[l : l + 1], nb_ref[l : l + 1])
        return (rows.astype(F32) + u).astype(BF16)

    head_load.wait()
    for m in range(M):
        pack(0, m, head_v[m])
    pl.semaphore_wait(barrier, len(peers))
    for m in range(M):
        ring_start(0, m)
    for copy in small_load:
        copy.wait()
    row = lax.broadcasted_iota(jnp.int32, (N, 2 * HALO), 0)
    halo = jnp.where(row == halo_ref[...], 1.0, 0.0).T
    o_halo[...] = halo.astype(BF16)
    node_load.wait()
    for m in range(M):
        rows = node_v[m]
        near_rows[0, m, 0:N] = rows
        halo_pack(0, m, rows)
        halo_start(0, m)
    for l in range(LAYERS):
        for i in range(4):
            weight_copy(l, i).start()
    for copy in long_load:
        copy.wait()
    coarse = long_v[...].astype(F32).astype(BF16)
    G = NX * NY * 2 * NZ
    for nb, o_pick in ((1, o_pick_one), (2, o_pick_two)):
        S = 2 * NZ // nb
        row = lax.broadcasted_iota(jnp.int32, (G, nd), 0)
        col = lax.broadcasted_iota(jnp.int32, (G, nd), 1)
        to = lax.rem(lax.div(row, S), NX * NY)
        want = dom_of(lax.div(to, NY), z, lax.rem(to, NY))
        spread = jnp.where(col == want, 1.0, 0.0).astype(BF16)
        every = lax.dot_general(
            spread, coarse, (((1,), (1,)), ((), ())), preferred_element_type=F32
        )
        row = lax.broadcasted_iota(jnp.int32, (G, 2 * NZ), 0)
        col = lax.broadcasted_iota(jnp.int32, (G, 2 * NZ), 1)
        own = lax.div(row, NX * NY * S) * S + lax.rem(row, S)
        mine = jnp.where(col == own, every, 0.0).astype(BF16)
        pick = dot(mine, jnp.ones((2 * NZ, 4 * S), BF16))
        row = lax.broadcasted_iota(jnp.int32, (G, 4 * S), 0)
        col = lax.broadcasted_iota(jnp.int32, (G, 4 * S), 1)
        pick = pick + (8 * lax.div(lax.rem(row, S), 2)).astype(F32)
        for h in range(2):
            o_pick[h] = jnp.where(
                col.astype(F32) == pick + float(COARSE * h), 1.0, 0.0
            ).astype(BF16)

    live = count_ref[0]
    table = lax.broadcasted_iota(jnp.int32, (K, E), 0)
    sent = senders_ref[...]
    o_near[...] = jnp.where(table == sent, 1.0, 0.0).T.astype(BF16)
    q = jnp.maximum(sent - K, 0)
    slot = lax.rem(q, 2)
    part = lax.div(q, 2)
    part_y = lax.rem(part, NY)
    part_z = lax.rem(lax.div(part, NY), NZ)
    part_x = lax.div(part, NY * NZ)
    apart = lax.rem(z + NZ - part_z, NZ)
    rank = jnp.zeros_like(apart)
    for k, d in enumerate(RING):
        rank = jnp.where(apart == d, k, rank)
    place = (part_x * NY + part_y) * (2 * NZ) + rank * 2 + slot
    place = jnp.where(sent >= K, place, -1)
    table = lax.broadcasted_iota(jnp.int32, (F, E), 0)
    o_far[...] = jnp.where(table == place, 1.0, 0.0).T.astype(BF16)
    table = lax.broadcasted_iota(jnp.int32, (N, E), 0)
    lane = lax.broadcasted_iota(jnp.int32, (N, E), 1)
    got = jnp.where((table == receivers_ref[...]) & (lane < live), 1.0, 0.0)
    o_sum[...] = got.astype(BF16)
    o_recv[...] = got.T.astype(BF16)
    for b in range(BATCHES[0]):
        for m in range(M):
            forward(0, m, b)
    edge_load.wait()
    for i in range(4):
        w_load[0, i].wait()
    weight_copy(0, 0).wait_recv()
    for m in range(M):
        own_part(0, m)
    for m in range(M):
        halo_wait(0, m)
        near_part(0, m)
    for i in range(1, 4):
        weight_copy(0, i).wait_recv()
    centre(0, w2e)
    centre(0, w2n)
    for m in range(M):
        node_part(0, m)
    for i in range(4):
        w_load[1, i].wait()
        weight_copy(1, i).wait_recv()
    centre(1, w2e)
    centre(1, w2n)
    for m in range(M):
        edges(0, m)
        new = nodes(0, m)
        pack(1, m, new[0:8])
        ring_start(1, m)
        near_rows[1, m, 0:N] = new
    for m in range(M):
        halo_pack(1, m, near_rows[1, m, 0:N])
        halo_start(1, m)
    own_part(1, 0)
    own_part(1, 1)
    node_part(1, 0)
    node_part(1, 1)
    forward(1, 0, 0)
    forward(1, 1, 0)
    for m in range(M):
        halo_wait(1, m)
        near_part(1, m)
    outs = []
    for m in range(M):
        edges(1, m)
        out = pltpu.make_async_copy(edge_v.at[m], edge_out.at[m], out_sem.at[m, 0])
        out.start()
        outs.append(out)
        node_v[m] = nodes(1, m)
        out = pltpu.make_async_copy(node_v.at[m], node_out.at[m], out_sem.at[m, 1])
        out.start()
        outs.append(out)
    for l in range(LAYERS):
        for i in range(4):
            weight_copy(l, i).wait_send()
        for m in range(M):
            for k in range(1, NZ):
                ring_copy(l, m, k).wait_send()
            for b in range(BATCHES[l]):
                for k in range(len(PLANE)):
                    plane_copy(l, m, b, k).wait_send()
            for side in range(2):
                halo_copy(l, m, side).wait_send()
    for out in outs:
        out.wait()


def publish(node_in, edge_in, node_out, edge_out, node_v, edge_v, in_sem, out_sem):
    M, E = edge_in.shape[:2]
    pieces = []
    for m in range(M):
        for h in range(2):
            rows = pl.ds(h * (E // 2), E // 2)
            pieces.append(
                (edge_in.at[m, rows], edge_v.at[2 * m + h], edge_out.at[m, rows])
            )
    pieces.append((node_in, node_v, node_out))
    ins = [
        pltpu.make_async_copy(a, b, in_sem.at[i]) for i, (a, b, c) in enumerate(pieces)
    ]
    outs = [
        pltpu.make_async_copy(b, c, out_sem.at[i]) for i, (a, b, c) in enumerate(pieces)
    ]
    for copy in ins:
        copy.start()
    for a, b in zip(ins, outs):
        a.wait()
        b.start()
    for copy in outs:
        copy.wait()


def per_device(
    node_latents,
    edge_latents,
    edge_senders,
    edge_receivers,
    edge_counts,
    halo_send,
    long_send,
    edge_first,
    edge_second,
    node_first,
    node_second,
    edge_gain,
    edge_shift,
    node_gain,
    node_shift,
):
    M, N, D = node_latents.shape
    E = edge_latents.shape[1]
    H = D // 2
    L = LAYERS
    nd = NX * NY * NZ
    K = N + 2 * HALO
    F = 2 * nd
    G = NX * NY * 2 * NZ
    hbm = pl.BlockSpec(memory_space=pl.ANY)
    DMA = pltpu.SemaphoreType.DMA
    node_state, edge_state = pl.pallas_call(
        functools.partial(kernel, (M, N, E, D)),
        out_shape=(
            jax.ShapeDtypeStruct((M, N, D), BF16),
            jax.ShapeDtypeStruct((M, E, D), BF16),
        ),
        in_specs=[hbm] * 15,
        out_specs=(hbm, hbm),
        scratch_shapes=[
            pltpu.VMEM((M, N, D), BF16),
            pltpu.VMEM((M, E, D), BF16),
            pltpu.VMEM((M, 8, D), BF16),
            pltpu.VMEM((2 * NZ, nd), jnp.int32),
            pltpu.SMEM((1,), jnp.int32),
            pltpu.VMEM((1, E), jnp.int32),
            pltpu.VMEM((1, E), jnp.int32),
            pltpu.VMEM((1, 2 * HALO), jnp.int32),
            pltpu.VMEM((L, D), F32),
            pltpu.VMEM((L, D), F32),
            pltpu.VMEM((L, D), F32),
            pltpu.VMEM((L, D), F32),
            pltpu.VMEM((L, 2, 3 * D, H), BF16),
            pltpu.VMEM((L, 2, D, H), BF16),
            pltpu.VMEM((L, 2, 2 * D, H), BF16),
            pltpu.VMEM((L, 2, D, H), BF16),
            pltpu.VMEM((L, M, K, D), BF16),
            pltpu.VMEM((L, M, NX * NY, 2 * NZ, D), BF16),
            pltpu.VMEM((L, M, 8, H), BF16),
            pltpu.VMEM((L, M, NZ, 8, H), BF16),
            pltpu.VMEM((L, M, NX * NY, 2 * NZ, D), BF16),
            pltpu.VMEM((L, M, 2, HALO, D), BF16),
            pltpu.VMEM((E, K), BF16),
            pltpu.VMEM((E, F), BF16),
            pltpu.VMEM((E, N), BF16),
            pltpu.VMEM((N, E), BF16),
            pltpu.VMEM((2 * HALO, N), BF16),
            pltpu.VMEM((2, G, 8 * NZ), BF16),
            pltpu.VMEM((2, G, 4 * NZ), BF16),
            pltpu.VMEM((M, E, D), F32),
            pltpu.VMEM((M, N, D), F32),
            pltpu.VMEM((E, D), BF16),
            DMA(()),
            DMA((2 + 4 * L,)),
            DMA((NZ,)),
            DMA((8,)),
            DMA((M, 2)),
            DMA((L, 4)),
            DMA((L, 4)),
            DMA((L, M, NZ)),
            DMA((L, M, NZ)),
            DMA((L, M, 2, len(PLANE))),
            DMA((L, M, 2, len(PLANE))),
            DMA((L, M, 2)),
            DMA((L, M, 2)),
        ],
        compiler_params=pltpu.CompilerParams(
            collective_id=0, has_side_effects=True, vmem_limit_bytes=56 * 1024 * 1024
        ),
    )(
        edge_counts,
        edge_senders.reshape(1, E),
        edge_receivers.reshape(1, E),
        halo_send.reshape(1, 2 * HALO),
        edge_gain,
        edge_shift,
        node_gain,
        node_shift,
        long_send.transpose(0, 2, 1),
        node_latents,
        edge_latents,
        edge_first,
        edge_second,
        node_first,
        node_second,
    )
    return pl.pallas_call(
        publish,
        out_shape=(
            jax.ShapeDtypeStruct((M, N, D), BF16),
            jax.ShapeDtypeStruct((M, E, D), BF16),
        ),
        in_specs=[hbm, hbm],
        out_specs=(hbm, hbm),
        scratch_shapes=[
            pltpu.VMEM((M, N, D), BF16),
            pltpu.VMEM((2 * M, E // 2, D), BF16),
            DMA((1 + 2 * M,)),
            DMA((1 + 2 * M,)),
        ],
    )(node_state, edge_state)


def solution(mesh):
    placed = (
        P("mem", "dom", None),
        P("mem", "dom", None),
        P("dom"),
        P("dom"),
        P("dom"),
        P("dom"),
        P(),
        P(None, None, "mem"),
        P(None, None, "mem"),
        P(None, None, "mem"),
        P(None, None, "mem"),
        P(),
        P(),
        P(),
        P(),
    )
    return jax.shard_map(
        per_device,
        mesh=mesh,
        in_specs=placed,
        out_specs=(P("mem", "dom", None), P("mem", "dom", None)),
        check_vma=False,
    )
```

```python
import functools

import jax
import jax.numpy as jnp
from jax import lax
from jax.experimental import pallas as pl
from jax.experimental.pallas import tpu as pltpu
from jax.sharding import PartitionSpec as P

NX, NZ, NY = 4, 8, 4
HALO = 16
LAYERS = 2
COARSE = 4
MESH = pl.DeviceIdType.MESH
F32 = jnp.float32
BF16 = jnp.bfloat16
RING = sorted(range(NZ), key=lambda d: (min(d, NZ - d), d))
BATCHES = (2, 1)
PLANE = sorted(
    [(i, j) for i in range(NX) for j in range(NY) if (i, j) != (0, 0)],
    key=lambda o: -(min(o[0], NX - o[0]) + min(o[1], NY - o[1])),
)


def dot(a, b):
    return jnp.dot(a, b, preferred_element_type=F32)


def silu(x):
    half = 0.5 * x
    return half * jnp.tanh(half) + half


def kernel(
    dims,
    count_hbm,
    senders_hbm,
    receivers_hbm,
    halo_hbm,
    eg_hbm,
    eb_hbm,
    ng_hbm,
    nb_hbm,
    long_hbm,
    node_hbm,
    edge_hbm,
    ef_hbm,
    es_hbm,
    nf_hbm,
    ns_hbm,
    node_out,
    edge_out,
    node_v,
    edge_v,
    head_v,
    long_v,
    count_ref,
    senders_ref,
    receivers_ref,
    halo_ref,
    eg_ref,
    eb_ref,
    ng_ref,
    nb_ref,
    w1e,
    w2e,
    w1n,
    w2n,
    near_rows,
    far_rows,
    ring_send,
    ring_recv,
    plane_send,
    halo_out,
    o_near,
    o_far,
    o_recv,
    o_sum,
    o_halo,
    o_pick_one,
    o_pick_two,
    pre_v,
    node_pre,
    hid_v,
    head_sem,
    load_sem,
    long_sem,
    small_sem,
    out_sem,
    w_send,
    w_recv,
    ring_ssem,
    ring_rsem,
    plane_ssem,
    plane_rsem,
    halo_ssem,
    halo_rsem,
):
    M, N, E, D = dims
    H = D // 2
    K = N + 2 * HALO
    dom = lax.axis_index("dom")
    mem = lax.axis_index("mem")
    y = lax.rem(dom, NY)
    z = lax.rem(lax.div(dom, NY), NZ)
    x = lax.div(dom, NY * NZ)

    def dom_of(a, b, c):
        return (a * NZ + b) * NY + c

    def along(d):
        return (dom_of(x, lax.rem(z + d, NZ), y), mem)

    def across(o):
        return (dom_of(lax.rem(x + o[0], NX), z, lax.rem(y + o[1], NY)), mem)

    nd = NX * NY * NZ
    after = (lax.rem(dom + 1, nd), mem)
    before = (lax.rem(dom + nd - 1, nd), mem)
    twin = (dom, 1 - mem)
    here = x * NY + y
    peers = [along(d) for d in RING[1:]] + [across(o) for o in PLANE]
    peers += [after, before, twin]
    barrier = pltpu.get_barrier_semaphore()
    for p in peers:
        pl.semaphore_signal(barrier, inc=1, device_id=p, device_id_type=MESH)

    weights = ((ef_hbm, w1e), (es_hbm, w2e), (nf_hbm, w1n), (ns_hbm, w2n))
    long_load = [
        pltpu.make_async_copy(
            long_hbm.at[dom_of(x, lax.rem(z + NZ - d, NZ), y)],
            long_v.at[pl.ds(2 * k, 2)],
            long_sem.at[k],
        )
        for k, d in enumerate(RING)
    ]
    small = (
        (count_hbm, count_ref),
        (senders_hbm, senders_ref),
        (receivers_hbm, receivers_ref),
        (halo_hbm, halo_ref),
        (eg_hbm, eg_ref),
        (eb_hbm, eb_ref),
        (ng_hbm, ng_ref),
        (nb_hbm, nb_ref),
    )
    small_load = [
        pltpu.make_async_copy(src, dst, small_sem.at[i])
        for i, (src, dst) in enumerate(small)
    ]
    for copy in small_load + long_load:
        copy.start()
    node_load = pltpu.make_async_copy(node_hbm, node_v, load_sem.at[0])
    edge_load = pltpu.make_async_copy(edge_hbm, edge_v, load_sem.at[1])
    head_load = pltpu.make_async_copy(node_hbm.at[:, pl.ds(0, 8)], head_v, head_sem)
    head_load.start()
    node_load.start()
    w_load = {}
    for l in range(LAYERS):
        for i, (src, dst) in enumerate(weights):
            w_load[l, i] = pltpu.make_async_copy(
                src.at[l], dst.at[l, mem], load_sem.at[2 + 4 * l + i]
            )
            w_load[l, i].start()
            if l == 0 and i == 0:
                edge_load.start()

    F = 2 * nd

    def ring_copy(l, m, k):
        return pltpu.make_async_remote_copy(
            src_ref=ring_send.at[l, m],
            dst_ref=ring_recv.at[l, m, k],
            send_sem=ring_ssem.at[l, m, k],
            recv_sem=ring_rsem.at[l, m, k],
            device_id=along(RING[k]),
            device_id_type=MESH,
        )

    def plane_copy(l, m, b, k):
        o = PLANE[k]
        there = lax.rem(x + o[0], NX) * NY + lax.rem(y + o[1], NY)
        rows = 2 * NZ // BATCHES[l]
        return pltpu.make_async_remote_copy(
            src_ref=plane_send.at[l, m, there, pl.ds(b * rows, rows)],
            dst_ref=far_rows.at[l, m, here, pl.ds(b * rows, rows)],
            send_sem=plane_ssem.at[l, m, b, k],
            recv_sem=plane_rsem.at[l, m, b, k],
            device_id=across(o),
            device_id_type=MESH,
        )

    def halo_copy(l, m, side):
        return pltpu.make_async_remote_copy(
            src_ref=halo_out.at[l, m, side],
            dst_ref=near_rows.at[l, m, pl.ds(N + (1 - side) * HALO, HALO)],
            send_sem=halo_ssem.at[l, m, side],
            recv_sem=halo_rsem.at[l, m, side],
            device_id=before if side == 0 else after,
            device_id_type=MESH,
        )

    def weight_copy(l, i):
        src, dst = weights[i]
        return pltpu.make_async_remote_copy(
            src_ref=src.at[l],
            dst_ref=dst.at[l, mem],
            send_sem=w_send.at[l, i],
            recv_sem=w_recv.at[l, i],
            device_id=twin,
            device_id_type=MESH,
        )

    def pack(l, m, rows):
        wide = rows.astype(F32)
        upper = pltpu.roll(wide[:, H:D], COARSE, 0)
        row = lax.broadcasted_iota(jnp.int32, (8, H), 0)
        packed = jnp.where(row < COARSE, wide[:, 0:H], upper).astype(BF16)
        ring_send[l, m] = packed
        ring_recv[l, m, 0] = packed

    def halo_pack(l, m, rows):
        out = dot(o_halo[...], rows).astype(BF16)
        halo_out[l, m, 0] = out[0:HALO]
        halo_out[l, m, 1] = out[HALO : 2 * HALO]

    def ring_start(l, m):
        for k in reversed(range(1, NZ)):
            ring_copy(l, m, k).start()

    def halo_start(l, m):
        for side in range(2):
            halo_copy(l, m, side).start()

    def forward(l, m, b):
        nb = BATCHES[l]
        o_pick = o_pick_one if nb == 1 else o_pick_two
        size = NZ // nb
        for k in range(max(b * size, 1), (b + 1) * size):
            ring_copy(l, m, k).wait_recv()
        got = ring_recv[l, m, b * size : (b + 1) * size].reshape(8 * size, H)
        S = 2 * size
        rows = slice(b * NX * NY * S, (b + 1) * NX * NY * S)
        for h in range(2):
            plane_send[l, m, :, b * S : (b + 1) * S, h * H : (h + 1) * H] = (
                dot(o_pick[h, rows], got).astype(BF16).reshape(NX * NY, S, H)
            )
        for k in range(len(PLANE)):
            plane_copy(l, m, b, k).start()
        far_rows[l, m, here, b * S : (b + 1) * S] = plane_send[
            l, m, here, b * S : (b + 1) * S
        ]

    def halo_wait(l, m):
        for side in range(2):
            halo_copy(l, m, side).wait_recv()

    def own_part(l, m):
        rows = near_rows[l, m, 0:N]
        for n in range(2):
            cols = slice(n * H, (n + 1) * H)
            own = dot(rows, w1e[l, n, 2 * D : 3 * D]).astype(BF16)
            pre_v[m, :, cols] = dot(edge_v[m], w1e[l, n, 0:D]) + dot(o_recv[...], own)

    def near_part(l, m):
        rows = near_rows[l, m]
        for n in range(2):
            cols = slice(n * H, (n + 1) * H)
            proj = dot(rows, w1e[l, n, D : 2 * D]).astype(BF16)
            pre_v[m, :, cols] += dot(o_near[...], proj)

    def node_part(l, m):
        rows = near_rows[l, m, 0:N]
        for n in range(2):
            node_pre[m, :, n * H : (n + 1) * H] = dot(rows, w1n[l, n, 0:D])

    def norm(v, gain, shift):
        var = jnp.mean(v * v, -1, keepdims=True)
        return v * lax.rsqrt(var + 1e-05) * gain + shift

    def centre(l, w):
        a, b = w[l, 0].astype(F32), w[l, 1].astype(F32)
        mean = jnp.sum(a + b, -1, keepdims=True) * (1.0 / D)
        w[l, 0] = (a - mean).astype(BF16)
        w[l, 1] = (b - mean).astype(BF16)

    CH = min(256, E)

    def edges(l, m):
        for b in range(BATCHES[l]):
            for k in range(len(PLANE)):
                plane_copy(l, m, b, k).wait_recv()
        rows = far_rows[l, m].reshape(F, D)
        for n in range(2):
            cols = slice(n * H, (n + 1) * H)
            proj = dot(rows, w1e[l, n, D : 2 * D]).astype(BF16)
            for c in range(E // CH):
                r = slice(c * CH, (c + 1) * CH)
                hid_v[r, cols] = silu(pre_v[m, r, cols] + dot(o_far[r], proj)).astype(BF16)
        gain = eg_ref[l : l + 1]
        shift = eb_ref[l : l + 1]
        for c in range(E // CH):
            r = slice(c * CH, (c + 1) * CH)
            h = hid_v[r]
            v = jnp.concatenate([dot(h, w2e[l, 0]), dot(h, w2e[l, 1])], -1)
            u = norm(v, gain, shift)
            at = lax.broadcasted_iota(jnp.int32, (CH, 1), 0) + c * CH
            edge_v[m, r] = jnp.where(
                at < live, edge_v[m, r].astype(F32) + u, 0.0
            ).astype(BF16)

    def nodes(l, m):
        summed = dot(o_sum[...], edge_v[m]).astype(BF16)
        rows = near_rows[l, m, 0:N]
        hid = []
        for n in range(2):
            a = node_pre[m, :, n * H : (n + 1) * H] + dot(summed, w1n[l, n, D : 2 * D])
            hid.append(silu(a).astype(BF16))
        h = jnp.concatenate(hid, -1)
        v = jnp.concatenate([dot(h, w2n[l, 0]), dot(h, w2n[l, 1])], -1)
        gain = ng_ref[l : l + 1]
        shift = nb_ref[l : l + 1]
        if l + 1 < LAYERS:
            pack(l + 1, m, (rows[0:8].astype(F32) + norm(v[0:8], gain, shift)).astype(BF16))
            ring_start(l + 1, m)
        return (rows.astype(F32) + norm(v, gain, shift)).astype(BF16)

    head_load.wait()
    for m in range(M):
        pack(0, m, head_v[m])
    pl.semaphore_wait(barrier, len(peers))
    for m in range(M):
        ring_start(0, m)
    for copy in small_load:
        copy.wait()
    row = lax.broadcasted_iota(jnp.int32, (N, 2 * HALO), 0)
    halo = jnp.where(row == halo_ref[...], 1.0, 0.0).T
    o_halo[...] = halo.astype(BF16)
    node_load.wait()
    for m in range(M):
        rows = node_v[m]
        near_rows[0, m, 0:N] = rows
        halo_pack(0, m, rows)
        halo_start(0, m)
    for l in range(LAYERS):
        for i in range(4):
            weight_copy(l, i).start()
    for copy in long_load:
        copy.wait()
    coarse = long_v[...].astype(F32).astype(BF16)
    G = NX * NY * 2 * NZ
    for nb, o_pick in ((1, o_pick_one), (2, o_pick_two)):
        S = 2 * NZ // nb
        row = lax.broadcasted_iota(jnp.int32, (G, nd), 0)
        col = lax.broadcasted_iota(jnp.int32, (G, nd), 1)
        to = lax.rem(lax.div(row, S), NX * NY)
        want = dom_of(lax.div(to, NY), z, lax.rem(to, NY))
        spread = jnp.where(col == want, 1.0, 0.0).astype(BF16)
        every = lax.dot_general(
            spread, coarse, (((1,), (1,)), ((), ())), preferred_element_type=F32
        )
        row = lax.broadcasted_iota(jnp.int32, (G, 2 * NZ), 0)
        col = lax.broadcasted_iota(jnp.int32, (G, 2 * NZ), 1)
        own = lax.div(row, NX * NY * S) * S + lax.rem(row, S)
        mine = jnp.where(col == own, every, 0.0).astype(BF16)
        pick = dot(mine, jnp.ones((2 * NZ, 4 * S), BF16))
        row = lax.broadcasted_iota(jnp.int32, (G, 4 * S), 0)
        col = lax.broadcasted_iota(jnp.int32, (G, 4 * S), 1)
        pick = pick + (8 * lax.div(lax.rem(row, S), 2)).astype(F32)
        for h in range(2):
            o_pick[h] = jnp.where(
                col.astype(F32) == pick + float(COARSE * h), 1.0, 0.0
            ).astype(BF16)

    live = count_ref[0]
    table = lax.broadcasted_iota(jnp.int32, (K, E), 0)
    sent = senders_ref[...]
    o_near[...] = jnp.where(table == sent, 1.0, 0.0).T.astype(BF16)
    q = jnp.maximum(sent - K, 0)
    slot = lax.rem(q, 2)
    part = lax.div(q, 2)
    part_y = lax.rem(part, NY)
    part_z = lax.rem(lax.div(part, NY), NZ)
    part_x = lax.div(part, NY * NZ)
    apart = lax.rem(z + NZ - part_z, NZ)
    rank = jnp.zeros_like(apart)
    for k, d in enumerate(RING):
        rank = jnp.where(apart == d, k, rank)
    place = (part_x * NY + part_y) * (2 * NZ) + rank * 2 + slot
    place = jnp.where(sent >= K, place, -1)
    table = lax.broadcasted_iota(jnp.int32, (F, E), 0)
    o_far[...] = jnp.where(table == place, 1.0, 0.0).T.astype(BF16)
    table = lax.broadcasted_iota(jnp.int32, (N, E), 0)
    lane = lax.broadcasted_iota(jnp.int32, (N, E), 1)
    got = jnp.where((table == receivers_ref[...]) & (lane < live), 1.0, 0.0)
    o_sum[...] = got.astype(BF16)
    o_recv[...] = got.T.astype(BF16)
    for b in range(BATCHES[0]):
        for m in range(M):
            forward(0, m, b)
    edge_load.wait()
    for i in range(4):
        w_load[0, i].wait()
    weight_copy(0, 0).wait_recv()
    for m in range(M):
        own_part(0, m)
    for m in range(M):
        halo_wait(0, m)
        near_part(0, m)
    for i in range(1, 4):
        weight_copy(0, i).wait_recv()
    centre(0, w2e)
    centre(0, w2n)
    for m in range(M):
        node_part(0, m)
    for i in range(4):
        w_load[1, i].wait()
        weight_copy(1, i).wait_recv()
    centre(1, w2e)
    centre(1, w2n)
    for m in range(M):
        edges(0, m)
        new = nodes(0, m)
        near_rows[1, m, 0:N] = new
    for m in range(M):
        halo_pack(1, m, near_rows[1, m, 0:N])
        halo_start(1, m)
    own_part(1, 0)
    own_part(1, 1)
    node_part(1, 0)
    node_part(1, 1)
    forward(1, 0, 0)
    forward(1, 1, 0)
    for m in range(M):
        halo_wait(1, m)
        near_part(1, m)
    outs = []
    for m in range(M):
        edges(1, m)
        out = pltpu.make_async_copy(edge_v.at[m], edge_out.at[m], out_sem.at[m, 0])
        out.start()
        outs.append(out)
        node_v[m] = nodes(1, m)
        out = pltpu.make_async_copy(node_v.at[m], node_out.at[m], out_sem.at[m, 1])
        out.start()
        outs.append(out)
    for l in range(LAYERS):
        for i in range(4):
            weight_copy(l, i).wait_send()
        for m in range(M):
            for k in range(1, NZ):
                ring_copy(l, m, k).wait_send()
            for b in range(BATCHES[l]):
                for k in range(len(PLANE)):
                    plane_copy(l, m, b, k).wait_send()
            for side in range(2):
                halo_copy(l, m, side).wait_send()
    for out in outs:
        out.wait()


def publish(node_in, edge_in, node_out, edge_out, node_v, edge_v, in_sem, out_sem):
    M, E = edge_in.shape[:2]
    pieces = []
    for m in range(M):
        for h in range(2):
            rows = pl.ds(h * (E // 2), E // 2)
            pieces.append(
                (edge_in.at[m, rows], edge_v.at[2 * m + h], edge_out.at[m, rows])
            )
    pieces.append((node_in, node_v, node_out))
    ins = [
        pltpu.make_async_copy(a, b, in_sem.at[i]) for i, (a, b, c) in enumerate(pieces)
    ]
    outs = [
        pltpu.make_async_copy(b, c, out_sem.at[i]) for i, (a, b, c) in enumerate(pieces)
    ]
    for copy in ins:
        copy.start()
    for a, b in zip(ins, outs):
        a.wait()
        b.start()
    for copy in outs:
        copy.wait()


def per_device(
    node_latents,
    edge_latents,
    edge_senders,
    edge_receivers,
    edge_counts,
    halo_send,
    long_send,
    edge_first,
    edge_second,
    node_first,
    node_second,
    edge_gain,
    edge_shift,
    node_gain,
    node_shift,
):
    M, N, D = node_latents.shape
    E = edge_latents.shape[1]
    H = D // 2
    L = LAYERS
    nd = NX * NY * NZ
    K = N + 2 * HALO
    F = 2 * nd
    G = NX * NY * 2 * NZ
    hbm = pl.BlockSpec(memory_space=pl.ANY)
    DMA = pltpu.SemaphoreType.DMA
    node_state, edge_state = pl.pallas_call(
        functools.partial(kernel, (M, N, E, D)),
        out_shape=(
            jax.ShapeDtypeStruct((M, N, D), BF16),
            jax.ShapeDtypeStruct((M, E, D), BF16),
        ),
        in_specs=[hbm] * 15,
        out_specs=(hbm, hbm),
        scratch_shapes=[
            pltpu.VMEM((M, N, D), BF16),
            pltpu.VMEM((M, E, D), BF16),
            pltpu.VMEM((M, 8, D), BF16),
            pltpu.VMEM((2 * NZ, nd), jnp.int32),
            pltpu.SMEM((1,), jnp.int32),
            pltpu.VMEM((1, E), jnp.int32),
            pltpu.VMEM((1, E), jnp.int32),
            pltpu.VMEM((1, 2 * HALO), jnp.int32),
            pltpu.VMEM((L, D), F32),
            pltpu.VMEM((L, D), F32),
            pltpu.VMEM((L, D), F32),
            pltpu.VMEM((L, D), F32),
            pltpu.VMEM((L, 2, 3 * D, H), BF16),
            pltpu.VMEM((L, 2, D, H), BF16),
            pltpu.VMEM((L, 2, 2 * D, H), BF16),
            pltpu.VMEM((L, 2, D, H), BF16),
            pltpu.VMEM((L, M, K, D), BF16),
            pltpu.VMEM((L, M, NX * NY, 2 * NZ, D), BF16),
            pltpu.VMEM((L, M, 8, H), BF16),
            pltpu.VMEM((L, M, NZ, 8, H), BF16),
            pltpu.VMEM((L, M, NX * NY, 2 * NZ, D), BF16),
            pltpu.VMEM((L, M, 2, HALO, D), BF16),
            pltpu.VMEM((E, K), BF16),
            pltpu.VMEM((E, F), BF16),
            pltpu.VMEM((E, N), BF16),
            pltpu.VMEM((N, E), BF16),
            pltpu.VMEM((2 * HALO, N), BF16),
            pltpu.VMEM((2, G, 8 * NZ), BF16),
            pltpu.VMEM((2, G, 4 * NZ), BF16),
            pltpu.VMEM((M, E, D), F32),
            pltpu.VMEM((M, N, D), F32),
            pltpu.VMEM((E, D), BF16),
            DMA(()),
            DMA((2 + 4 * L,)),
            DMA((NZ,)),
            DMA((8,)),
            DMA((M, 2)),
            DMA((L, 4)),
            DMA((L, 4)),
            DMA((L, M, NZ)),
            DMA((L, M, NZ)),
            DMA((L, M, 2, len(PLANE))),
            DMA((L, M, 2, len(PLANE))),
            DMA((L, M, 2)),
            DMA((L, M, 2)),
        ],
        compiler_params=pltpu.CompilerParams(
            collective_id=0, has_side_effects=True, vmem_limit_bytes=56 * 1024 * 1024
        ),
    )(
        edge_counts,
        edge_senders.reshape(1, E),
        edge_receivers.reshape(1, E),
        halo_send.reshape(1, 2 * HALO),
        edge_gain,
        edge_shift,
        node_gain,
        node_shift,
        long_send.transpose(0, 2, 1),
        node_latents,
        edge_latents,
        edge_first,
        edge_second,
        node_first,
        node_second,
    )
    return pl.pallas_call(
        publish,
        out_shape=(
            jax.ShapeDtypeStruct((M, N, D), BF16),
            jax.ShapeDtypeStruct((M, E, D), BF16),
        ),
        in_specs=[hbm, hbm],
        out_specs=(hbm, hbm),
        scratch_shapes=[
            pltpu.VMEM((M, N, D), BF16),
            pltpu.VMEM((2 * M, E // 2, D), BF16),
            DMA((1 + 2 * M,)),
            DMA((1 + 2 * M,)),
        ],
    )(node_state, edge_state)


def solution(mesh):
    placed = (
        P("mem", "dom", None),
        P("mem", "dom", None),
        P("dom"),
        P("dom"),
        P("dom"),
        P("dom"),
        P(),
        P(None, None, "mem"),
        P(None, None, "mem"),
        P(None, None, "mem"),
        P(None, None, "mem"),
        P(),
        P(),
        P(),
        P(),
    )
    return jax.shard_map(
        per_device,
        mesh=mesh,
        in_specs=placed,
        out_specs=(P("mem", "dom", None), P("mem", "dom", None)),
        check_vma=False,
    )
```

```python
import functools

import jax
import jax.numpy as jnp
from jax import lax
from jax.experimental import pallas as pl
from jax.experimental.pallas import tpu as pltpu
from jax.sharding import PartitionSpec as P

NX, NZ, NY = 4, 8, 4
HALO = 16
LAYERS = 2
COARSE = 4
MESH = pl.DeviceIdType.MESH
F32 = jnp.float32
BF16 = jnp.bfloat16
RING = sorted(range(NZ), key=lambda d: (min(d, NZ - d), d))
BATCHES = (2, 1)
PLANE = sorted(
    [(i, j) for i in range(NX) for j in range(NY) if (i, j) != (0, 0)],
    key=lambda o: -(min(o[0], NX - o[0]) + min(o[1], NY - o[1])),
)


def dot(a, b):
    return jnp.dot(a, b, preferred_element_type=F32)


def silu(x):
    half = 0.5 * x
    return half * jnp.tanh(half) + half


def kernel(
    dims,
    count_hbm,
    senders_hbm,
    receivers_hbm,
    halo_hbm,
    eg_hbm,
    eb_hbm,
    ng_hbm,
    nb_hbm,
    long_hbm,
    node_hbm,
    edge_hbm,
    ef_hbm,
    es_hbm,
    nf_hbm,
    ns_hbm,
    node_out,
    edge_out,
    node_v,
    edge_v,
    head_v,
    long_v,
    count_ref,
    senders_ref,
    receivers_ref,
    halo_ref,
    eg_ref,
    eb_ref,
    ng_ref,
    nb_ref,
    w1e,
    w2e,
    w1n,
    w2n,
    near_rows,
    far_rows,
    ring_send,
    ring_recv,
    plane_send,
    halo_out,
    o_near,
    o_far,
    o_recv,
    o_sum,
    o_halo,
    o_pick_one,
    o_pick_two,
    pre_v,
    node_pre,
    hid_v,
    head_sem,
    load_sem,
    long_sem,
    small_sem,
    out_sem,
    w_send,
    w_recv,
    ring_ssem,
    ring_rsem,
    plane_ssem,
    plane_rsem,
    halo_ssem,
    halo_rsem,
):
    M, N, E, D = dims
    H = D // 2
    K = N + 2 * HALO
    dom = lax.axis_index("dom")
    mem = lax.axis_index("mem")
    y = lax.rem(dom, NY)
    z = lax.rem(lax.div(dom, NY), NZ)
    x = lax.div(dom, NY * NZ)

    def dom_of(a, b, c):
        return (a * NZ + b) * NY + c

    def along(d):
        return (dom_of(x, lax.rem(z + d, NZ), y), mem)

    def across(o):
        return (dom_of(lax.rem(x + o[0], NX), z, lax.rem(y + o[1], NY)), mem)

    nd = NX * NY * NZ
    after = (lax.rem(dom + 1, nd), mem)
    before = (lax.rem(dom + nd - 1, nd), mem)
    twin = (dom, 1 - mem)
    here = x * NY + y
    peers = [along(d) for d in RING[1:]] + [across(o) for o in PLANE]
    peers += [after, before, twin]
    barrier = pltpu.get_barrier_semaphore()
    for p in peers:
        pl.semaphore_signal(barrier, inc=1, device_id=p, device_id_type=MESH)

    weights = ((ef_hbm, w1e), (es_hbm, w2e), (nf_hbm, w1n), (ns_hbm, w2n))
    long_load = [
        pltpu.make_async_copy(
            long_hbm.at[dom_of(x, lax.rem(z + NZ - d, NZ), y)],
            long_v.at[pl.ds(2 * k, 2)],
            long_sem.at[k],
        )
        for k, d in enumerate(RING)
    ]
    small = (
        (count_hbm, count_ref),
        (senders_hbm, senders_ref),
        (receivers_hbm, receivers_ref),
        (halo_hbm, halo_ref),
        (eg_hbm, eg_ref),
        (eb_hbm, eb_ref),
        (ng_hbm, ng_ref),
        (nb_hbm, nb_ref),
    )
    small_load = [
        pltpu.make_async_copy(src, dst, small_sem.at[i])
        for i, (src, dst) in enumerate(small)
    ]
    for copy in small_load + long_load:
        copy.start()
    node_load = pltpu.make_async_copy(node_hbm, node_v, load_sem.at[0])
    edge_load = pltpu.make_async_copy(edge_hbm, edge_v, load_sem.at[1])
    head_load = pltpu.make_async_copy(node_hbm.at[:, pl.ds(0, 8)], head_v, head_sem)
    head_load.start()
    node_load.start()
    w_load = {}
    for l in range(LAYERS):
        for i, (src, dst) in enumerate(weights):
            w_load[l, i] = pltpu.make_async_copy(
                src.at[l], dst.at[l, mem], load_sem.at[2 + 4 * l + i]
            )
            w_load[l, i].start()
            if l == 0 and i == 0:
                edge_load.start()

    F = 2 * nd

    def ring_copy(l, m, k):
        return pltpu.make_async_remote_copy(
            src_ref=ring_send.at[l, m],
            dst_ref=ring_recv.at[l, m, k],
            send_sem=ring_ssem.at[l, m, k],
            recv_sem=ring_rsem.at[l, m, k],
            device_id=along(RING[k]),
            device_id_type=MESH,
        )

    def plane_copy(l, m, b, k):
        o = PLANE[k]
        there = lax.rem(x + o[0], NX) * NY + lax.rem(y + o[1], NY)
        rows = 2 * NZ // BATCHES[l]
        return pltpu.make_async_remote_copy(
            src_ref=plane_send.at[l, m, there, pl.ds(b * rows, rows)],
            dst_ref=far_rows.at[l, m, here, pl.ds(b * rows, rows)],
            send_sem=plane_ssem.at[l, m, b, k],
            recv_sem=plane_rsem.at[l, m, b, k],
            device_id=across(o),
            device_id_type=MESH,
        )

    def halo_copy(l, m, side):
        return pltpu.make_async_remote_copy(
            src_ref=halo_out.at[l, m, side],
            dst_ref=near_rows.at[l, m, pl.ds(N + (1 - side) * HALO, HALO)],
            send_sem=halo_ssem.at[l, m, side],
            recv_sem=halo_rsem.at[l, m, side],
            device_id=before if side == 0 else after,
            device_id_type=MESH,
        )

    def weight_copy(l, i):
        src, dst = weights[i]
        return pltpu.make_async_remote_copy(
            src_ref=src.at[l],
            dst_ref=dst.at[l, mem],
            send_sem=w_send.at[l, i],
            recv_sem=w_recv.at[l, i],
            device_id=twin,
            device_id_type=MESH,
        )

    def pack(l, m, rows):
        wide = rows.astype(F32)
        upper = pltpu.roll(wide[:, H:D], COARSE, 0)
        row = lax.broadcasted_iota(jnp.int32, (8, H), 0)
        packed = jnp.where(row < COARSE, wide[:, 0:H], upper).astype(BF16)
        ring_send[l, m] = packed
        ring_recv[l, m, 0] = packed

    def halo_pack(l, m, rows):
        out = dot(o_halo[...], rows).astype(BF16)
        halo_out[l, m, 0] = out[0:HALO]
        halo_out[l, m, 1] = out[HALO : 2 * HALO]

    def ring_start(l, m):
        for k in reversed(range(1, NZ)):
            ring_copy(l, m, k).start()

    def halo_start(l, m):
        for side in range(2):
            halo_copy(l, m, side).start()

    def forward(l, m, b):
        nb = BATCHES[l]
        o_pick = o_pick_one if nb == 1 else o_pick_two
        size = NZ // nb
        for k in range(max(b * size, 1), (b + 1) * size):
            ring_copy(l, m, k).wait_recv()
        got = ring_recv[l, m, b * size : (b + 1) * size].reshape(8 * size, H)
        S = 2 * size
        rows = slice(b * NX * NY * S, (b + 1) * NX * NY * S)
        for h in range(2):
            plane_send[l, m, :, b * S : (b + 1) * S, h * H : (h + 1) * H] = (
                dot(o_pick[h, rows], got).astype(BF16).reshape(NX * NY, S, H)
            )
        for k in range(len(PLANE)):
            plane_copy(l, m, b, k).start()
        far_rows[l, m, here, b * S : (b + 1) * S] = plane_send[
            l, m, here, b * S : (b + 1) * S
        ]

    def halo_wait(l, m):
        for side in range(2):
            halo_copy(l, m, side).wait_recv()

    def own_part(l, m):
        rows = near_rows[l, m, 0:N]
        for n in range(2):
            cols = slice(n * H, (n + 1) * H)
            own = dot(rows, w1e[l, n, 2 * D : 3 * D]).astype(BF16)
            pre_v[m, :, cols] = dot(edge_v[m], w1e[l, n, 0:D]) + dot(o_recv[...], own)

    def near_part(l, m):
        rows = near_rows[l, m]
        for n in range(2):
            cols = slice(n * H, (n + 1) * H)
            proj = dot(rows, w1e[l, n, D : 2 * D]).astype(BF16)
            pre_v[m, :, cols] += dot(o_near[...], proj)

    def node_part(l, m):
        rows = near_rows[l, m, 0:N]
        for n in range(2):
            node_pre[m, :, n * H : (n + 1) * H] = dot(rows, w1n[l, n, 0:D])

    def norm(v, gain, shift):
        var = jnp.mean(v * v, -1, keepdims=True)
        return v * lax.rsqrt(var + 1e-05) * gain + shift

    def centre(l, w):
        a, b = w[l, 0].astype(F32), w[l, 1].astype(F32)
        mean = jnp.sum(a + b, -1, keepdims=True) * (1.0 / D)
        w[l, 0] = (a - mean).astype(BF16)
        w[l, 1] = (b - mean).astype(BF16)

    CH = min(256, E)

    def edges(l, m):
        for b in range(BATCHES[l]):
            for k in range(len(PLANE)):
                plane_copy(l, m, b, k).wait_recv()
        rows = far_rows[l, m].reshape(F, D)
        for n in range(2):
            cols = slice(n * H, (n + 1) * H)
            proj = dot(rows, w1e[l, n, D : 2 * D]).astype(BF16)
            for c in range(E // CH):
                r = slice(c * CH, (c + 1) * CH)
                hid_v[r, cols] = silu(pre_v[m, r, cols] + dot(o_far[r], proj)).astype(BF16)
        gain = eg_ref[l : l + 1]
        shift = eb_ref[l : l + 1]
        for c in range(E // CH):
            r = slice(c * CH, (c + 1) * CH)
            h = hid_v[r]
            v = jnp.concatenate([dot(h, w2e[l, 0]), dot(h, w2e[l, 1])], -1)
            u = norm(v, gain, shift)
            at = lax.broadcasted_iota(jnp.int32, (CH, 1), 0) + c * CH
            edge_v[m, r] = jnp.where(
                at < live, edge_v[m, r].astype(F32) + u, 0.0
            ).astype(BF16)

    def nodes(l, m):
        summed = dot(o_sum[...], edge_v[m]).astype(BF16)
        rows = near_rows[l, m, 0:N]
        hid = []
        for n in range(2):
            a = node_pre[m, :, n * H : (n + 1) * H] + dot(summed, w1n[l, n, D : 2 * D])
            hid.append(silu(a).astype(BF16))
        h = jnp.concatenate(hid, -1)
        v = jnp.concatenate([dot(h, w2n[l, 0]), dot(h, w2n[l, 1])], -1)
        gain = ng_ref[l : l + 1]
        shift = nb_ref[l : l + 1]
        if l + 1 < LAYERS:
            pack(l + 1, m, (rows[0:8].astype(F32) + norm(v[0:8], gain, shift)).astype(BF16))
            ring_start(l + 1, m)
        return (rows.astype(F32) + norm(v, gain, shift)).astype(BF16)

    head_load.wait()
    for m in range(M):
        pack(0, m, head_v[m])
    pl.semaphore_wait(barrier, len(peers))
    for m in range(M):
        ring_start(0, m)
    for copy in small_load:
        copy.wait()
    row = lax.broadcasted_iota(jnp.int32, (N, 2 * HALO), 0)
    halo = jnp.where(row == halo_ref[...], 1.0, 0.0).T
    o_halo[...] = halo.astype(BF16)
    node_load.wait()
    for m in range(M):
        rows = node_v[m]
        near_rows[0, m, 0:N] = rows
        halo_pack(0, m, rows)
        halo_start(0, m)
    for l in range(LAYERS):
        for i in range(4):
            weight_copy(l, i).start()
    for copy in long_load:
        copy.wait()
    coarse = long_v[...].astype(F32).astype(BF16)
    G = NX * NY * 2 * NZ
    for nb, o_pick in ((1, o_pick_one), (2, o_pick_two)):
        S = 2 * NZ // nb
        row = lax.broadcasted_iota(jnp.int32, (G, nd), 0)
        col = lax.broadcasted_iota(jnp.int32, (G, nd), 1)
        to = lax.rem(lax.div(row, S), NX * NY)
        want = dom_of(lax.div(to, NY), z, lax.rem(to, NY))
        spread = jnp.where(col == want, 1.0, 0.0).astype(BF16)
        every = lax.dot_general(
            spread, coarse, (((1,), (1,)), ((), ())), preferred_element_type=F32
        )
        row = lax.broadcasted_iota(jnp.int32, (G, 2 * NZ), 0)
        col = lax.broadcasted_iota(jnp.int32, (G, 2 * NZ), 1)
        own = lax.div(row, NX * NY * S) * S + lax.rem(row, S)
        mine = jnp.where(col == own, every, 0.0).astype(BF16)
        pick = dot(mine, jnp.ones((2 * NZ, 4 * S), BF16))
        row = lax.broadcasted_iota(jnp.int32, (G, 4 * S), 0)
        col = lax.broadcasted_iota(jnp.int32, (G, 4 * S), 1)
        pick = pick + (8 * lax.div(lax.rem(row, S), 2)).astype(F32)
        for h in range(2):
            o_pick[h] = jnp.where(
                col.astype(F32) == pick + float(COARSE * h), 1.0, 0.0
            ).astype(BF16)

    for b in range(BATCHES[0]):
        for m in range(M):
            forward(0, m, b)
    live = count_ref[0]
    table = lax.broadcasted_iota(jnp.int32, (K, E), 0)
    sent = senders_ref[...]
    o_near[...] = jnp.where(table == sent, 1.0, 0.0).T.astype(BF16)
    q = jnp.maximum(sent - K, 0)
    slot = lax.rem(q, 2)
    part = lax.div(q, 2)
    part_y = lax.rem(part, NY)
    part_z = lax.rem(lax.div(part, NY), NZ)
    part_x = lax.div(part, NY * NZ)
    apart = lax.rem(z + NZ - part_z, NZ)
    rank = jnp.zeros_like(apart)
    for k, d in enumerate(RING):
        rank = jnp.where(apart == d, k, rank)
    place = (part_x * NY + part_y) * (2 * NZ) + rank * 2 + slot
    place = jnp.where(sent >= K, place, -1)
    table = lax.broadcasted_iota(jnp.int32, (F, E), 0)
    o_far[...] = jnp.where(table == place, 1.0, 0.0).T.astype(BF16)
    table = lax.broadcasted_iota(jnp.int32, (N, E), 0)
    lane = lax.broadcasted_iota(jnp.int32, (N, E), 1)
    got = jnp.where((table == receivers_ref[...]) & (lane < live), 1.0, 0.0)
    o_sum[...] = got.astype(BF16)
    o_recv[...] = got.T.astype(BF16)
    edge_load.wait()
    for i in range(4):
        w_load[0, i].wait()
    weight_copy(0, 0).wait_recv()
    for m in range(M):
        own_part(0, m)
    for m in range(M):
        halo_wait(0, m)
        near_part(0, m)
    for i in range(1, 4):
        weight_copy(0, i).wait_recv()
    centre(0, w2e)
    centre(0, w2n)
    for m in range(M):
        node_part(0, m)
    for i in range(4):
        w_load[1, i].wait()
        weight_copy(1, i).wait_recv()
    centre(1, w2e)
    centre(1, w2n)
    for m in range(M):
        edges(0, m)
        new = nodes(0, m)
        near_rows[1, m, 0:N] = new
    for m in range(M):
        halo_pack(1, m, near_rows[1, m, 0:N])
        halo_start(1, m)
    own_part(1, 0)
    own_part(1, 1)
    node_part(1, 0)
    node_part(1, 1)
    forward(1, 0, 0)
    forward(1, 1, 0)
    for m in range(M):
        halo_wait(1, m)
        near_part(1, m)
    outs = []
    for m in range(M):
        edges(1, m)
        out = pltpu.make_async_copy(edge_v.at[m], edge_out.at[m], out_sem.at[m, 0])
        out.start()
        outs.append(out)
        node_v[m] = nodes(1, m)
        out = pltpu.make_async_copy(node_v.at[m], node_out.at[m], out_sem.at[m, 1])
        out.start()
        outs.append(out)
    for l in range(LAYERS):
        for i in range(4):
            weight_copy(l, i).wait_send()
        for m in range(M):
            for k in range(1, NZ):
                ring_copy(l, m, k).wait_send()
            for b in range(BATCHES[l]):
                for k in range(len(PLANE)):
                    plane_copy(l, m, b, k).wait_send()
            for side in range(2):
                halo_copy(l, m, side).wait_send()
    for out in outs:
        out.wait()


def publish(node_in, edge_in, node_out, edge_out, node_v, edge_v, in_sem, out_sem):
    M, E = edge_in.shape[:2]
    pieces = []
    for m in range(M):
        for h in range(2):
            rows = pl.ds(h * (E // 2), E // 2)
            pieces.append(
                (edge_in.at[m, rows], edge_v.at[2 * m + h], edge_out.at[m, rows])
            )
    pieces.append((node_in, node_v, node_out))
    ins = [
        pltpu.make_async_copy(a, b, in_sem.at[i]) for i, (a, b, c) in enumerate(pieces)
    ]
    outs = [
        pltpu.make_async_copy(b, c, out_sem.at[i]) for i, (a, b, c) in enumerate(pieces)
    ]
    for copy in ins:
        copy.start()
    for a, b in zip(ins, outs):
        a.wait()
        b.start()
    for copy in outs:
        copy.wait()


def per_device(
    node_latents,
    edge_latents,
    edge_senders,
    edge_receivers,
    edge_counts,
    halo_send,
    long_send,
    edge_first,
    edge_second,
    node_first,
    node_second,
    edge_gain,
    edge_shift,
    node_gain,
    node_shift,
):
    M, N, D = node_latents.shape
    E = edge_latents.shape[1]
    H = D // 2
    L = LAYERS
    nd = NX * NY * NZ
    K = N + 2 * HALO
    F = 2 * nd
    G = NX * NY * 2 * NZ
    hbm = pl.BlockSpec(memory_space=pl.ANY)
    DMA = pltpu.SemaphoreType.DMA
    node_state, edge_state = pl.pallas_call(
        functools.partial(kernel, (M, N, E, D)),
        out_shape=(
            jax.ShapeDtypeStruct((M, N, D), BF16),
            jax.ShapeDtypeStruct((M, E, D), BF16),
        ),
        in_specs=[hbm] * 15,
        out_specs=(hbm, hbm),
        scratch_shapes=[
            pltpu.VMEM((M, N, D), BF16),
            pltpu.VMEM((M, E, D), BF16),
            pltpu.VMEM((M, 8, D), BF16),
            pltpu.VMEM((2 * NZ, nd), jnp.int32),
            pltpu.SMEM((1,), jnp.int32),
            pltpu.VMEM((1, E), jnp.int32),
            pltpu.VMEM((1, E), jnp.int32),
            pltpu.VMEM((1, 2 * HALO), jnp.int32),
            pltpu.VMEM((L, D), F32),
            pltpu.VMEM((L, D), F32),
            pltpu.VMEM((L, D), F32),
            pltpu.VMEM((L, D), F32),
            pltpu.VMEM((L, 2, 3 * D, H), BF16),
            pltpu.VMEM((L, 2, D, H), BF16),
            pltpu.VMEM((L, 2, 2 * D, H), BF16),
            pltpu.VMEM((L, 2, D, H), BF16),
            pltpu.VMEM((L, M, K, D), BF16),
            pltpu.VMEM((L, M, NX * NY, 2 * NZ, D), BF16),
            pltpu.VMEM((L, M, 8, H), BF16),
            pltpu.VMEM((L, M, NZ, 8, H), BF16),
            pltpu.VMEM((L, M, NX * NY, 2 * NZ, D), BF16),
            pltpu.VMEM((L, M, 2, HALO, D), BF16),
            pltpu.VMEM((E, K), BF16),
            pltpu.VMEM((E, F), BF16),
            pltpu.VMEM((E, N), BF16),
            pltpu.VMEM((N, E), BF16),
            pltpu.VMEM((2 * HALO, N), BF16),
            pltpu.VMEM((2, G, 8 * NZ), BF16),
            pltpu.VMEM((2, G, 4 * NZ), BF16),
            pltpu.VMEM((M, E, D), F32),
            pltpu.VMEM((M, N, D), F32),
            pltpu.VMEM((E, D), BF16),
            DMA(()),
            DMA((2 + 4 * L,)),
            DMA((NZ,)),
            DMA((8,)),
            DMA((M, 2)),
            DMA((L, 4)),
            DMA((L, 4)),
            DMA((L, M, NZ)),
            DMA((L, M, NZ)),
            DMA((L, M, 2, len(PLANE))),
            DMA((L, M, 2, len(PLANE))),
            DMA((L, M, 2)),
            DMA((L, M, 2)),
        ],
        compiler_params=pltpu.CompilerParams(
            collective_id=0, has_side_effects=True, vmem_limit_bytes=56 * 1024 * 1024
        ),
    )(
        edge_counts,
        edge_senders.reshape(1, E),
        edge_receivers.reshape(1, E),
        halo_send.reshape(1, 2 * HALO),
        edge_gain,
        edge_shift,
        node_gain,
        node_shift,
        long_send.transpose(0, 2, 1),
        node_latents,
        edge_latents,
        edge_first,
        edge_second,
        node_first,
        node_second,
    )
    return pl.pallas_call(
        publish,
        out_shape=(
            jax.ShapeDtypeStruct((M, N, D), BF16),
            jax.ShapeDtypeStruct((M, E, D), BF16),
        ),
        in_specs=[hbm, hbm],
        out_specs=(hbm, hbm),
        scratch_shapes=[
            pltpu.VMEM((M, N, D), BF16),
            pltpu.VMEM((2 * M, E // 2, D), BF16),
            DMA((1 + 2 * M,)),
            DMA((1 + 2 * M,)),
        ],
    )(node_state, edge_state)


def solution(mesh):
    placed = (
        P("mem", "dom", None),
        P("mem", "dom", None),
        P("dom"),
        P("dom"),
        P("dom"),
        P("dom"),
        P(),
        P(None, None, "mem"),
        P(None, None, "mem"),
        P(None, None, "mem"),
        P(None, None, "mem"),
        P(),
        P(),
        P(),
        P(),
    )
    return jax.shard_map(
        per_device,
        mesh=mesh,
        in_specs=placed,
        out_specs=(P("mem", "dom", None), P("mem", "dom", None)),
        check_vma=False,
    )
```
